8 devices in a mesh: cz: 2 (over z, y), cy: 2 (over x), cx: 2 (over core).
Axes of the slice: x: 2, y: 2, z: 1, core: 2. Of those that a mesh axis runs over, the one named last changes fastest.
Arguments:
- x: bfloat16 [768, 3072], P(('cx', 'cz'), 'cy')
- w1: bfloat16 [3072, 12288], P('cy', ('cz', 'cx'))
- w2: bfloat16 [12288, 3072], P('cz', ('cy', 'cx'))
Outputs:
- output: bfloat16 [768, 3072], P(('cx', 'cz'), 'cy')
All inputs are finite; a program needn't handle non-finite values.
Results may differ from the reference program's by a relative error of at most 0.0115081.
Values are sent between devices in bfloat16 or wider.
A program may use at most 1 GiB of HBM per device.

```python
import jax
import jax.numpy as jnp

N = 768
D = 3072
F = 12288


def setup_inputs(seed: int = 0) -> dict:
    k1, k2, k3 = jax.random.split(jax.random.PRNGKey(seed), 3)
    x = jax.random.normal(k1, (N, D), jnp.float32)
    w1 = jax.random.normal(k2, (D, F), jnp.float32) * D ** -0.5
    w2 = jax.random.normal(k3, (F, D), jnp.float32) * F ** -0.5
    return {"x": x.astype(jnp.bfloat16), "w1": w1.astype(jnp.bfloat16), "w2": w2.astype(jnp.bfloat16)}


def reference(x, w1, w2):
    c = jnp.dot(x, w1, preferred_element_type=jnp.float32).astype(jnp.bfloat16)
    h = jax.nn.gelu(c.astype(jnp.float32), approximate=True).astype(jnp.bfloat16)
    return jnp.dot(h, w2, preferred_element_type=jnp.float32).astype(jnp.bfloat16)
```

```python
import math

import jax
import jax.numpy as jnp
from jax import lax
from jax.experimental import pallas as pl
from jax.experimental.pallas import tpu as pltpu
from jax.sharding import PartitionSpec as P

MESH = pl.DeviceIdType.MESH
F32 = jnp.float32
BF16 = jnp.bfloat16
M = 64
TILE = 512


def gelu_tanh(c):
    return 0.5 * c * (1.0 + jnp.tanh(math.sqrt(2 / math.pi) * (c + 0.044715 * (c * c * c))))


def kernel(x, w1, w2, z, xv, w1v, w2v, ps, pr, po, ho, hr, zs, zr, ov,
           xl_sem, w1_sem, w2_sem, out_sem, bx_send, bx_recv, bw_send, bw_recv,
           xy_send, xy_recv, xf_send, xf_recv, p_send, p_recv, h_send, h_recv, z_send, z_recv):
    cz, cy, cx = lax.axis_index("cz"), lax.axis_index("cy"), lax.axis_index("cx")
    across = {"cy": 1 - cy}
    partner = {"cx": 1 - cx}
    along = {"cz": 1 - cz}
    diagonal = {"cz": 1 - cz, "cx": 1 - cx}
    rows, half = x.shape
    chunks = 4 * rows // M
    per = rows // M

    def remote(src, dst, send, recv, device):
        return pltpu.make_async_remote_copy(src_ref=src, dst_ref=dst, send_sem=send, recv_sem=recv,
                                            device_id=device, device_id_type=MESH)

    def at(i, n=M):
        return pl.ds(pl.multiple_of(i * M, M), n)

    x_first = pltpu.make_async_copy(x.at[pl.ds(0, M)], xv.at[pl.ds(0, M)], xl_sem.at[0])
    x_last = pltpu.make_async_copy(x.at[pl.ds(M, rows - M)], xv.at[pl.ds(10 * M, rows - M)], xl_sem.at[1])
    cols = lambda side: pl.ds(pl.multiple_of(side * half, half), half)
    w1_send = pltpu.make_async_copy(w1.at[:, cols(1 - cy)], w1v.at[0], w1_sem.at[0])
    w1_keep = pltpu.make_async_copy(w1.at[:, cols(cy)], w1v.at[1], w1_sem.at[1])
    width = w2.shape[1]

    def w2_rows(core, k):
        side = cy if k == 0 else 1 - cy
        return w2.at[pl.ds(pl.multiple_of((core * 2 + side) * half, half), half)]

    mine = pl.ds(pl.multiple_of(cx * width, width), width)
    w2_local = [pltpu.make_async_copy(w2_rows(cx, k), w2v.at[k, :, mine], w2_sem.at[k]) for k in range(2)]
    w2_swap = [remote(w2_rows(1 - cx, k), w2v.at[k, :, mine], bw_send.at[k], bw_recv.at[k], partner) for k in range(2)]
    x_swap = [
        remote(x.at[pl.ds(0, M)], xv.at[pl.ds(M, M)], bx_send.at[0], bx_recv.at[0], partner),
        remote(x.at[pl.ds(M, rows - M)], xv.at[pl.ds(8 * M, rows - M)], bx_send.at[1], bx_recv.at[1], partner),
    ]
    x_along = [remote(x.at[pl.ds(k * M, M)], xv.at[pl.ds((2 + k) * M, M)], xy_send.at[k], xy_recv.at[k], along)
               for k in range(per)]

    def x_forward(k):
        return remote(xv.at[at(2 + k)], xv.at[at(5 + k)], xf_send.at[k], xf_recv.at[k], partner)

    def p_copy(i):
        return remote(ps.at[at(i)], pr.at[at(i)], p_send.at[i], p_recv.at[i], across)

    def h_copy(i):
        return remote(ho.at[at(i)], hr.at[at(i)], h_send.at[i], h_recv.at[i], across)

    def z_copy(i, slot, row, device):
        return remote(zs.at[at(i)], zr.at[slot, at(row)], z_send.at[i], z_recv.at[i], device)

    x_first.start()
    w1_send.start()
    x_last.start()
    w1_keep.start()

    barrier = pltpu.get_barrier_semaphore()
    for device in (across, partner, along, diagonal):
        pl.semaphore_signal(barrier, inc=1, device_id=device, device_id_type=MESH)
    pl.semaphore_wait(barrier, 4)

    for copy in x_along:
        copy.start()
    for copy in x_swap:
        copy.start()

    def first_layer(i, side, out, out_rows):
        for n in range(half // TILE):
            c = pl.ds(n * TILE, TILE)
            out[out_rows, c] = jnp.dot(xv[at(i), :], w1v[side, :, c], preferred_element_type=F32)

    def partial(i):
        @pl.when(i == 0)
        def _():
            x_first.wait()
            w1_send.wait()

        @pl.when(i == 1)
        def _():
            x_swap[0].wait_recv()

        @pl.when((i >= 2) & (i < 5))
        def _():
            k = i - 2
            remote(xv.at[at(i)], xv.at[at(i)], xy_send.at[k], xy_recv.at[k], along).wait_recv()
            x_forward(k).start()

        @pl.when((i >= 5) & (i < 8))
        def _():
            x_forward(i - 5).wait_recv()

        @pl.when(i == 8)
        def _():
            x_swap[1].wait_recv()

        @pl.when(i == 10)
        def _():
            x_last.wait()

        first_layer(i, 0, ps, at(i))
        p_copy(i).start()

        @pl.when(i == 0)
        def _():
            w1_keep.wait()
            for copy in w2_local:
                copy.start()
            for copy in w2_swap:
                copy.start()

    def hidden(i):
        first_layer(i, 1, po, pl.ds(0, M))
        p_copy(i).wait_recv()
        for n in range(half // TILE):
            c = pl.ds(n * TILE, TILE)
            c_in = (po[:, c] + pr[at(i), c]).astype(BF16).astype(F32)
            ho[at(i), c] = gelu_tanh(c_in).astype(BF16)
        h_copy(i).start()

    def second_layer(i):
        @pl.when(i == 0)
        def _():
            for copy in w2_local:
                copy.wait()
            for copy in w2_swap:
                copy.wait_recv()

        for n in range(half // TILE):
            c = pl.ds(n * TILE, TILE)
            zs[at(i), c] = jnp.dot(ho[at(i), :], w2v[0, :, c], preferred_element_type=F32)
        h_copy(i).wait_recv()
        for n in range(half // TILE):
            c = pl.ds(n * TILE, TILE)
            zs[at(i), c] += jnp.dot(hr[at(i), :], w2v[1, :, c], preferred_element_type=F32)

        @pl.when(i == 1)
        def _():
            z_copy(i, 0, 0, partner).start()

        @pl.when((i >= 2) & (i < 5))
        def _():
            z_copy(i, 1, i - 2, along).start()

        @pl.when((i >= 5) & (i < 8))
        def _():
            z_copy(i, 2, i - 5, diagonal).start()

        @pl.when((i >= 8) & (i < 10))
        def _():
            z_copy(i, 0, i - 7, partner).start()

    def step(t, carry):
        @pl.when((t >= 2) & (t < chunks + 2))
        def _():
            hidden(t - 2)

        @pl.when(t < chunks)
        def _():
            partial(t)

        @pl.when(t >= 3)
        def _():
            second_layer(t - 3)

        return carry

    lax.fori_loop(0, chunks + 3, step, 0)

    came = {0: (1, 2, 5), 1: (8, 3, 6), 2: (9, 4, 7)}
    outs = []
    for r in range(per):
        for slot, i in enumerate(came[r]):
            z_copy(i, slot, r, (partner, along, diagonal)[slot]).wait_recv()
        own = pl.ds((0, 10, 11)[r] * M, M)
        row = pl.ds(r * M, M)
        ov[row, :] = (zs[own, :] + zr[0, row, :] + zr[1, row, :] + zr[2, row, :]).astype(BF16)
        outs.append(pltpu.make_async_copy(ov.at[row], z.at[row], out_sem.at[r]))
        outs[-1].start()

    for copy in x_along + x_swap + w2_swap:
        copy.wait_send()
    for k in range(per):
        x_forward(k).wait_send()
    for i in range(chunks):
        p_copy(i).wait_send()
        h_copy(i).wait_send()
    for i in range(1, 10):
        z_copy(i, 0, 0, partner).wait_send()
    for copy in outs:
        copy.wait()


def solution(mesh):
    def body(x, w1, w2):
        rows, half = x.shape
        total, chunks = 4 * rows, 4 * rows // M
        dma = lambda n: pltpu.SemaphoreType.DMA((n,))
        return pl.pallas_call(
            kernel,
            out_shape=jax.ShapeDtypeStruct((rows, half), BF16),
            in_specs=[pl.BlockSpec(memory_space=pl.ANY)] * 3,
            out_specs=pl.BlockSpec(memory_space=pl.ANY),
            scratch_shapes=[
                pltpu.VMEM((total, half), BF16),
                pltpu.VMEM((2, half, half), BF16),
                pltpu.VMEM((2, half, half), BF16),
                pltpu.VMEM((total, half), F32),
                pltpu.VMEM((total, half), F32),
                pltpu.VMEM((M, half), F32),
                pltpu.VMEM((total, half), BF16),
                pltpu.VMEM((total, half), BF16),
                pltpu.VMEM((total, half), F32),
                pltpu.VMEM((3, rows, half), F32),
                pltpu.VMEM((rows, half), BF16),
                dma(2), dma(2), dma(2), dma(3),
                dma(2), dma(2), dma(2), dma(2),
                dma(3), dma(3), dma(3), dma(3),
                dma(chunks), dma(chunks), dma(chunks), dma(chunks), dma(chunks), dma(chunks),
            ],
            compiler_params=pltpu.CompilerParams(
                collective_id=0, has_side_effects=True, vmem_limit_bytes=60 * 1024 * 1024
            ),
        )(x, w1, w2)

    return jax.shard_map(
        body,
        mesh=mesh,
        in_specs=(P(("cx", "cz"), "cy"), P("cy", ("cz", "cx")), P("cz", ("cy", "cx"))),
        out_specs=P(("cx", "cz"), "cy"),
        check_vma=False,
    )
```

```python
import math

import jax
import jax.numpy as jnp
from jax import lax
from jax.experimental import pallas as pl
from jax.experimental.pallas import tpu as pltpu
from jax.sharding import PartitionSpec as P

MESH = pl.DeviceIdType.MESH
F32 = jnp.float32
BF16 = jnp.bfloat16
M = 64
TILE = 512
PIECES = ((0, 512), (512, 512), (1024, 256), (1280, 256))


def gelu_tanh(c):
    return 0.5 * c * (1.0 + jnp.tanh(math.sqrt(2 / math.pi) * (c + 0.044715 * (c * c * c))))


def kernel(x, w1, w2, z, xv, w1v, w2v, ps, pr, po, ho, hr, zs, zr,
           xl_sem, w1_sem, w2_sem, bx_send, bx_recv, bw_send, bw_recv,
           xy_send, xy_recv, xf_send, xf_recv, p_send, p_recv, h_send, h_recv, z_send, z_recv):
    cz, cy, cx = lax.axis_index("cz"), lax.axis_index("cy"), lax.axis_index("cx")
    across = {"cy": 1 - cy}
    partner = {"cx": 1 - cx}
    along = {"cz": 1 - cz}
    diagonal = {"cz": 1 - cz, "cx": 1 - cx}
    rows, half = x.shape
    chunks = 4 * rows // M
    per = rows // M

    def remote(src, dst, send, recv, device):
        return pltpu.make_async_remote_copy(src_ref=src, dst_ref=dst, send_sem=send, recv_sem=recv,
                                            device_id=device, device_id_type=MESH)

    def at(i, n=M):
        return pl.ds(pl.multiple_of(i * M, M), n)

    x_first = pltpu.make_async_copy(x.at[pl.ds(0, M)], xv.at[pl.ds(0, M)], xl_sem.at[0])
    x_last = pltpu.make_async_copy(x.at[pl.ds(M, rows - M)], xv.at[pl.ds(10 * M, rows - M)], xl_sem.at[1])
    tiles = half // TILE

    def w1_cols(side, n):
        return w1.at[:, pl.ds(pl.multiple_of(side * half + n * TILE, TILE), TILE)]

    w1_send = [pltpu.make_async_copy(w1_cols(1 - cy, n), w1v.at[0, :, pl.ds(n * TILE, TILE)], w1_sem.at[n])
               for n in range(tiles)]
    w1_keep = pltpu.make_async_copy(w1.at[:, pl.ds(pl.multiple_of(cy * half, half), half)], w1v.at[1], w1_sem.at[tiles])
    width = w2.shape[1]

    def w2_rows(core, k):
        side = cy if k == 0 else 1 - cy
        return w2.at[pl.ds(pl.multiple_of((core * 2 + side) * half, half), half)]

    mine = pl.ds(pl.multiple_of(cx * width, width), width)
    w2_local = [pltpu.make_async_copy(w2_rows(cx, k), w2v.at[k, :, mine], w2_sem.at[k]) for k in range(2)]
    w2_swap = [remote(w2_rows(1 - cx, k), w2v.at[k, :, mine], bw_send.at[k], bw_recv.at[k], partner) for k in range(2)]
    x_swap = [
        remote(x.at[pl.ds(0, M)], xv.at[pl.ds(M, M)], bx_send.at[0], bx_recv.at[0], partner),
        remote(x.at[pl.ds(M, rows - M)], xv.at[pl.ds(8 * M, rows - M)], bx_send.at[1], bx_recv.at[1], partner),
    ]
    x_along = [remote(x.at[pl.ds(k * M, M)], xv.at[pl.ds((2 + k) * M, M)], xy_send.at[k], xy_recv.at[k], along)
               for k in range(per)]

    def x_forward(k):
        return remote(xv.at[at(2 + k)], xv.at[at(5 + k)], xf_send.at[k], xf_recv.at[k], partner)

    def p_copy(i):
        return remote(ps.at[at(i)], pr.at[at(i)], p_send.at[i], p_recv.at[i], across)

    def h_copy(i):
        return remote(ho.at[at(i)], hr.at[at(i)], h_send.at[i], h_recv.at[i], across)

    def z_copy(i, slot, row, device):
        return remote(zs.at[at(i)], zr.at[slot, at(row)], z_send.at[i], z_recv.at[i], device)

    def h_piece(k):
        c = pl.ds(*PIECES[k])
        return remote(ho.at[at(chunks - 1), c], hr.at[at(chunks - 1), c],
                      h_send.at[chunks - 1 + k], h_recv.at[chunks - 1 + k], across)

    barrier = pltpu.get_barrier_semaphore()
    for device in (across, partner, along, diagonal):
        pl.semaphore_signal(barrier, inc=1, device_id=device, device_id_type=MESH)

    x_first.start()
    for copy in w1_send:
        copy.start()
    x_first.wait()
    for n in range(tiles):
        c = pl.ds(n * TILE, TILE)
        w1_send[n].wait()
        ps[pl.ds(0, M), c] = jnp.dot(xv[pl.ds(0, M), :], w1v[0, :, c], preferred_element_type=F32)
    x_last.start()
    w1_keep.start()
    for copy in w2_local:
        copy.start()

    pl.semaphore_wait(barrier, 4)
    p_copy(0).start()
    x_swap[0].start()
    for copy in x_along:
        copy.start()
    x_swap[1].start()
    for copy in w2_swap:
        copy.start()
    w1_keep.wait()

    def first_layer(i, side, out, out_rows):
        for n in range(half // TILE):
            c = pl.ds(n * TILE, TILE)
            out[out_rows, c] = jnp.dot(xv[at(i), :], w1v[side, :, c], preferred_element_type=F32)

    def partial(i):
        @pl.when(i == 1)
        def _():
            x_swap[0].wait_recv()

        @pl.when((i >= 2) & (i < 5))
        def _():
            k = i - 2
            remote(xv.at[at(i)], xv.at[at(i)], xy_send.at[k], xy_recv.at[k], along).wait_recv()
            x_forward(k).start()

        @pl.when((i >= 5) & (i < 8))
        def _():
            x_forward(i - 5).wait_recv()

        @pl.when(i == 8)
        def _():
            x_swap[1].wait_recv()

        @pl.when(i == 10)
        def _():
            x_last.wait()

        first_layer(i, 0, ps, at(i))
        p_copy(i).start()

    def activate(i, c):
        total = (po[:, c] + pr[at(i), c]).astype(BF16).astype(F32)
        ho[at(i), c] = gelu_tanh(total).astype(BF16)

    def hidden(i):
        first_layer(i, 1, po, pl.ds(0, M))
        p_copy(i).wait_recv()
        for n in range(tiles):
            activate(i, pl.ds(n * TILE, TILE))
        h_copy(i).start()

    def second_own(i):
        for n in range(tiles):
            c = pl.ds(n * TILE, TILE)
            zs[at(i), c] = jnp.dot(ho[at(i), :], w2v[0, :, c], preferred_element_type=F32)

    def second_other(i):
        h_copy(i).wait_recv()
        for n in range(tiles):
            c = pl.ds(n * TILE, TILE)
            zs[at(i), c] += jnp.dot(hr[at(i), :], w2v[1, :, c], preferred_element_type=F32)

    def second_layer(i):
        @pl.when(i == 0)
        def _():
            for copy in w2_local:
                copy.wait()
            for copy in w2_swap:
                copy.wait_recv()

        second_own(i)
        second_other(i)

        @pl.when(i == 1)
        def _():
            z_copy(i, 0, 0, partner).start()

        @pl.when((i >= 2) & (i < 5))
        def _():
            z_copy(i, 1, i - 2, along).start()

        @pl.when((i >= 5) & (i < 8))
        def _():
            z_copy(i, 2, i - 5, diagonal).start()

        @pl.when((i >= 8) & (i < 10))
        def _():
            z_copy(i, 0, i - 7, partner).start()

    def step(t, carry):
        @pl.when(t >= 2)
        def _():
            hidden(t - 2)

        @pl.when(t < chunks)
        def _():
            partial(t)

        @pl.when(t >= 3)
        def _():
            second_layer(t - 3)

        return carry

    lax.fori_loop(1, chunks + 1, step, 0)

    last = chunks - 1
    first_layer(last, 1, po, pl.ds(0, M))
    p_copy(last).wait_recv()
    for k, piece in enumerate(PIECES):
        activate(last, pl.ds(*piece))
        h_piece(k).start()
    second_own(last)
    second_own(last - 1)

    def others(r):
        came = ((1, 2, 5), (8, 3, 6), (9, 4, 7))[r]
        for slot, i in enumerate(came):
            z_copy(i, slot, r, (partner, along, diagonal)[slot]).wait_recv()
        row = pl.ds(r * M, M)
        return row, lambda c: zr[0, row, c] + zr[1, row, c] + zr[2, row, c]

    def finish(r, i):
        row, came = others(r)
        for n in range(tiles):
            c = pl.ds(n * TILE, TILE)
            z[row, c] = (zs[at(i), c] + came(c)).astype(BF16)

    finish(0, 0)
    row, came = others(2)
    for n in range(tiles):
        c = pl.ds(n * TILE, TILE)
        zs[at(last), c] += came(c)
    second_other(last - 1)
    finish(1, last - 1)
    for k, (start, width) in enumerate(PIECES):
        h_piece(k).wait_recv()
        for n in range(tiles):
            c = pl.ds(n * TILE, TILE)
            total = zs[at(last), c] + jnp.dot(
                hr[at(last), pl.ds(start, width)], w2v[1, pl.ds(start, width), c], preferred_element_type=F32)
            if k < len(PIECES) - 1:
                zs[at(last), c] = total
            else:
                z[row, c] = total.astype(BF16)

    for copy in x_along + x_swap + w2_swap:
        copy.wait_send()
    for k in range(per):
        x_forward(k).wait_send()
    for i in range(chunks):
        p_copy(i).wait_send()
    for i in range(chunks - 1):
        h_copy(i).wait_send()
    for k in range(len(PIECES)):
        h_piece(k).wait_send()
    for i in range(1, 10):
        z_copy(i, 0, 0, partner).wait_send()


def solution(mesh):
    def body(x, w1, w2):
        rows, half = x.shape
        total, chunks = 4 * rows, 4 * rows // M
        dma = lambda n: pltpu.SemaphoreType.DMA((n,))
        last = chunks - 1 + len(PIECES)
        return pl.pallas_call(
            kernel,
            out_shape=jax.ShapeDtypeStruct((rows, half), BF16),
            in_specs=[pl.BlockSpec(memory_space=pl.ANY)] * 3,
            out_specs=pl.BlockSpec(memory_space=pltpu.VMEM),
            scratch_shapes=[
                pltpu.VMEM((total, half), BF16),
                pltpu.VMEM((2, half, half), BF16),
                pltpu.VMEM((2, half, half), BF16),
                pltpu.VMEM((total, half), F32),
                pltpu.VMEM((total, half), F32),
                pltpu.VMEM((M, half), F32),
                pltpu.VMEM((total, half), BF16),
                pltpu.VMEM((total, half), BF16),
                pltpu.VMEM((total, half), F32),
                pltpu.VMEM((3, rows, half), F32),
                dma(2), dma(half // TILE + 1), dma(2),
                dma(2), dma(2), dma(2), dma(2),
                dma(3), dma(3), dma(3), dma(3),
                dma(chunks), dma(chunks), dma(last), dma(last), dma(chunks), dma(chunks),
            ],
            compiler_params=pltpu.CompilerParams(
                collective_id=0, has_side_effects=True, vmem_limit_bytes=48 * 1024 * 1024
            ),
        )(pltpu.with_memory_space_constraint(x, pltpu.HBM), w1, w2)

    return jax.shard_map(
        body,
        mesh=mesh,
        in_specs=(P(("cx", "cz"), "cy"), P("cy", ("cz", "cx")), P("cz", ("cy", "cx"))),
        out_specs=P(("cx", "cz"), "cy"),
        check_vma=False,
    )
```

```python
import math

import jax
import jax.numpy as jnp
from jax import lax
from jax.experimental import pallas as pl
from jax.experimental.pallas import tpu as pltpu
from jax.sharding import PartitionSpec as P

MESH = pl.DeviceIdType.MESH
F32 = jnp.float32
BF16 = jnp.bfloat16
M = 64
TILE = 512
FIRST = ((0, 256), (256, 256), (512, 512), (1024, 512))
PIECES = ((0, 512), (512, 512), (1024, 256), (1280, 256))


def gelu_tanh(c):
    return 0.5 * c * (1.0 + jnp.tanh(math.sqrt(2 / math.pi) * (c + 0.044715 * (c * c * c))))


def kernel(x, w1, w2, z, xv, w1v, w2v, ps, pr, po, ho, hr, zs, zr,
           xl_sem, w1_sem, w2_sem, bx_send, bx_recv, bw_send, bw_recv,
           xy_send, xy_recv, xf_send, xf_recv, p_send, p_recv, h_send, h_recv, z_send, z_recv):
    cz, cy, cx = lax.axis_index("cz"), lax.axis_index("cy"), lax.axis_index("cx")
    across = {"cy": 1 - cy}
    partner = {"cx": 1 - cx}
    along = {"cz": 1 - cz}
    diagonal = {"cz": 1 - cz, "cx": 1 - cx}
    rows, half = x.shape
    chunks = 4 * rows // M
    per = rows // M

    def remote(src, dst, send, recv, device):
        return pltpu.make_async_remote_copy(src_ref=src, dst_ref=dst, send_sem=send, recv_sem=recv,
                                            device_id=device, device_id_type=MESH)

    def at(i, n=M):
        return pl.ds(pl.multiple_of(i * M, M), n)

    x_first = pltpu.make_async_copy(x.at[pl.ds(0, M)], xv.at[pl.ds(0, M)], xl_sem.at[0])
    x_last = pltpu.make_async_copy(x.at[pl.ds(M, rows - M)], xv.at[pl.ds(10 * M, rows - M)], xl_sem.at[1])
    tiles = half // TILE

    parts = len(FIRST)

    def w1_cols(side, start, width):
        return w1.at[:, pl.ds(pl.multiple_of(side * half + start, 128), width)]

    w1_send = [pltpu.make_async_copy(w1_cols(1 - cy, *piece), w1v.at[0, :, pl.ds(*piece)], w1_sem.at[k])
               for k, piece in enumerate(FIRST)]
    w1_keep = pltpu.make_async_copy(w1_cols(cy, 0, half), w1v.at[1], w1_sem.at[parts])
    width = w2.shape[1]

    def w2_rows(core, k):
        side = cy if k == 0 else 1 - cy
        return w2.at[pl.ds(pl.multiple_of((core * 2 + side) * half, half), half)]

    mine = pl.ds(pl.multiple_of(cx * width, width), width)
    w2_local = [pltpu.make_async_copy(w2_rows(cx, k), w2v.at[k, :, mine], w2_sem.at[k]) for k in range(2)]
    w2_swap = [remote(w2_rows(1 - cx, k), w2v.at[k, :, mine], bw_send.at[k], bw_recv.at[k], partner) for k in range(2)]
    x_swap = [
        remote(x.at[pl.ds(0, M)], xv.at[pl.ds(M, M)], bx_send.at[0], bx_recv.at[0], partner),
        remote(x.at[pl.ds(M, rows - M)], xv.at[pl.ds(8 * M, rows - M)], bx_send.at[1], bx_recv.at[1], partner),
    ]
    x_along = [remote(x.at[pl.ds(k * M, M)], xv.at[pl.ds((2 + k) * M, M)], xy_send.at[k], xy_recv.at[k], along)
               for k in range(per)]

    def x_forward(k):
        return remote(xv.at[at(2 + k)], xv.at[at(5 + k)], xf_send.at[k], xf_recv.at[k], partner)

    def p_copy(i):
        return remote(ps.at[at(i)], pr.at[at(i)], p_send.at[i], p_recv.at[i], across)

    def h_copy(i):
        return remote(ho.at[at(i)], hr.at[at(i)], h_send.at[i], h_recv.at[i], across)

    def z_copy(i, slot, row, device):
        return remote(zs.at[at(i)], zr.at[slot, at(row)], z_send.at[i], z_recv.at[i], device)

    def p_piece(k):
        c = pl.ds(*FIRST[k])
        sem = k if k == 0 else chunks - 1 + k
        return remote(ps.at[pl.ds(0, M), c], pr.at[pl.ds(0, M), c], p_send.at[sem], p_recv.at[sem], across)

    def h_piece(k):
        c = pl.ds(*PIECES[k])
        return remote(ho.at[at(chunks - 1), c], hr.at[at(chunks - 1), c],
                      h_send.at[chunks - 1 + k], h_recv.at[chunks - 1 + k], across)

    barrier = pltpu.get_barrier_semaphore()
    for device in (across, partner, along, diagonal):
        pl.semaphore_signal(barrier, inc=1, device_id=device, device_id_type=MESH)

    x_first.start()
    w1_send[0].start()
    x_first.wait()
    for k in range(parts):
        c = pl.ds(*FIRST[k])
        w1_send[k].wait()
        if k == 0:
            w1_send[1].start()
        if k < parts - 2:
            w1_send[k + 2].start()
        ps[pl.ds(0, M), c] = jnp.dot(xv[pl.ds(0, M), :], w1v[0, :, c], preferred_element_type=F32)
        if k == 0:
            pl.semaphore_wait(barrier, 4)
        p_piece(k).start()

    x_last.start()
    w1_keep.start()
    for copy in w2_local:
        copy.start()
    x_swap[0].start()
    for copy in x_along:
        copy.start()
    x_swap[1].start()
    for copy in w2_swap:
        copy.start()
    w1_keep.wait()

    def first_layer(i, side, out, out_rows):
        for n in range(half // TILE):
            c = pl.ds(n * TILE, TILE)
            out[out_rows, c] = jnp.dot(xv[at(i), :], w1v[side, :, c], preferred_element_type=F32)

    def partial(i):
        @pl.when(i == 1)
        def _():
            x_swap[0].wait_recv()

        @pl.when((i >= 2) & (i < 5))
        def _():
            k = i - 2
            remote(xv.at[at(i)], xv.at[at(i)], xy_send.at[k], xy_recv.at[k], along).wait_recv()
            x_forward(k).start()

        @pl.when((i >= 5) & (i < 8))
        def _():
            x_forward(i - 5).wait_recv()

        @pl.when(i == 8)
        def _():
            x_swap[1].wait_recv()

        @pl.when(i == 10)
        def _():
            x_last.wait()

        first_layer(i, 0, ps, at(i))
        p_copy(i).start()

    def activate(i, c):
        total = (po[:, c] + pr[at(i), c]).astype(BF16).astype(F32)
        ho[at(i), c] = gelu_tanh(total).astype(BF16)

    def hidden(i):
        first_layer(i, 1, po, pl.ds(0, M))

        @pl.when(i == 0)
        def _():
            for k in range(parts):
                p_piece(k).wait_recv()

        @pl.when(i > 0)
        def _():
            p_copy(i).wait_recv()

        for n in range(tiles):
            activate(i, pl.ds(n * TILE, TILE))
        h_copy(i).start()

    def second_own(i):
        for n in range(tiles):
            c = pl.ds(n * TILE, TILE)
            zs[at(i), c] = jnp.dot(ho[at(i), :], w2v[0, :, c], preferred_element_type=F32)

    def second_other(i):
        h_copy(i).wait_recv()
        for n in range(tiles):
            c = pl.ds(n * TILE, TILE)
            zs[at(i), c] += jnp.dot(hr[at(i), :], w2v[1, :, c], preferred_element_type=F32)

    def second_layer(i):
        @pl.when(i == 0)
        def _():
            for copy in w2_local:
                copy.wait()
            for copy in w2_swap:
                copy.wait_recv()

        second_own(i)
        second_other(i)

        @pl.when(i == 1)
        def _():
            z_copy(i, 0, 0, partner).start()

        @pl.when((i >= 2) & (i < 5))
        def _():
            z_copy(i, 1, i - 2, along).start()

        @pl.when((i >= 5) & (i < 8))
        def _():
            z_copy(i, 2, i - 5, diagonal).start()

        @pl.when((i >= 8) & (i < 10))
        def _():
            z_copy(i, 0, i - 7, partner).start()

    def step(t, carry):
        @pl.when(t >= 2)
        def _():
            hidden(t - 2)

        @pl.when(t < chunks)
        def _():
            partial(t)

        @pl.when(t >= 3)
        def _():
            second_layer(t - 3)

        return carry

    lax.fori_loop(1, chunks + 1, step, 0)

    last = chunks - 1
    first_layer(last, 1, po, pl.ds(0, M))
    p_copy(last).wait_recv()
    for k, piece in enumerate(PIECES):
        activate(last, pl.ds(*piece))
        h_piece(k).start()
    second_own(last)
    second_own(last - 1)

    def others(r):
        came = ((1, 2, 5), (8, 3, 6), (9, 4, 7))[r]
        for slot, i in enumerate(came):
            z_copy(i, slot, r, (partner, along, diagonal)[slot]).wait_recv()
        row = pl.ds(r * M, M)
        return row, lambda c: zr[0, row, c] + zr[1, row, c] + zr[2, row, c]

    def finish(r, i):
        row, came = others(r)
        for n in range(tiles):
            c = pl.ds(n * TILE, TILE)
            z[row, c] = (zs[at(i), c] + came(c)).astype(BF16)

    finish(0, 0)
    row, came = others(2)
    for n in range(tiles):
        c = pl.ds(n * TILE, TILE)
        zs[at(last), c] += came(c)
    second_other(last - 1)
    finish(1, last - 1)
    for k, (start, width) in enumerate(PIECES):
        h_piece(k).wait_recv()
        for n in range(tiles):
            c = pl.ds(n * TILE, TILE)
            total = zs[at(last), c] + jnp.dot(
                hr[at(last), pl.ds(start, width)], w2v[1, pl.ds(start, width), c], preferred_element_type=F32)
            if k < len(PIECES) - 1:
                zs[at(last), c] = total
            else:
                z[row, c] = total.astype(BF16)

    for copy in x_along + x_swap + w2_swap:
        copy.wait_send()
    for k in range(per):
        x_forward(k).wait_send()
    for k in range(parts):
        p_piece(k).wait_send()
    for i in range(1, chunks):
        p_copy(i).wait_send()
    for i in range(chunks - 1):
        h_copy(i).wait_send()
    for k in range(len(PIECES)):
        h_piece(k).wait_send()
    for i in range(1, 10):
        z_copy(i, 0, 0, partner).wait_send()


def solution(mesh):
    def body(x, w1, w2):
        rows, half = x.shape
        total, chunks = 4 * rows, 4 * rows // M
        dma = lambda n: pltpu.SemaphoreType.DMA((n,))
        first, last = chunks - 1 + len(FIRST), chunks - 1 + len(PIECES)
        return pl.pallas_call(
            kernel,
            out_shape=jax.ShapeDtypeStruct((rows, half), BF16),
            in_specs=[pl.BlockSpec(memory_space=pl.ANY)] * 3,
            out_specs=pl.BlockSpec(memory_space=pltpu.VMEM),
            scratch_shapes=[
                pltpu.VMEM((total, half), BF16),
                pltpu.VMEM((2, half, half), BF16),
                pltpu.VMEM((2, half, half), BF16),
                pltpu.VMEM((total, half), F32),
                pltpu.VMEM((total, half), F32),
                pltpu.VMEM((M, half), F32),
                pltpu.VMEM((total, half), BF16),
                pltpu.VMEM((total, half), BF16),
                pltpu.VMEM((total, half), F32),
                pltpu.VMEM((3, rows, half), F32),
                dma(2), dma(len(FIRST) + 1), dma(2),
                dma(2), dma(2), dma(2), dma(2),
                dma(3), dma(3), dma(3), dma(3),
                dma(first), dma(first), dma(last), dma(last), dma(chunks), dma(chunks),
            ],
            compiler_params=pltpu.CompilerParams(
                collective_id=0, has_side_effects=True, vmem_limit_bytes=48 * 1024 * 1024
            ),
        )(pltpu.with_memory_space_constraint(x, pltpu.HBM), w1, w2)

    return jax.shard_map(
        body,
        mesh=mesh,
        in_specs=(P(("cx", "cz"), "cy"), P("cy", ("cz", "cx")), P("cz", ("cy", "cx"))),
        out_specs=P(("cx", "cz"), "cy"),
        check_vma=False,
    )
```

```python
import math

import jax
import jax.numpy as jnp
from jax import lax
from jax.experimental import pallas as pl
from jax.experimental.pallas import tpu as pltpu
from jax.sharding import PartitionSpec as P

MESH = pl.DeviceIdType.MESH
F32 = jnp.float32
BF16 = jnp.bfloat16
M = 64
TILE = 512
FIRST = ((0, 256), (256, 256), (512, 512), (1024, 512))
PIECES = ((0, 512), (512, 512), (1024, 256), (1280, 256))
DETOUR = 256


def gelu_tanh(c):
    return 0.5 * c * (1.0 + jnp.tanh(math.sqrt(2 / math.pi) * (c + 0.044715 * (c * c * c))))


def kernel(x, w1, w2, z, xv, w1v, w2v, ps, pr, po, ho, hr, zs, zr, ra, rb, rc,
           xl_sem, w1_sem, w2_sem, bx_send, bx_recv, bw_send, bw_recv,
           xy_send, xy_recv, xf_send, xf_recv, p_send, p_recv, h_send, h_recv, z_send, z_recv, r_send, r_recv):
    cz, cy, cx = lax.axis_index("cz"), lax.axis_index("cy"), lax.axis_index("cx")
    across = {"cy": 1 - cy}
    partner = {"cx": 1 - cx}
    along = {"cz": 1 - cz}
    diagonal = {"cz": 1 - cz, "cx": 1 - cx}
    rows, half = x.shape
    chunks = 4 * rows // M
    per = rows // M

    def remote(src, dst, send, recv, device):
        return pltpu.make_async_remote_copy(src_ref=src, dst_ref=dst, send_sem=send, recv_sem=recv,
                                            device_id=device, device_id_type=MESH)

    def at(i, n=M):
        return pl.ds(pl.multiple_of(i * M, M), n)

    last = chunks - 1
    detours = (cz == 0) & (cx == 0)
    relays = (cz == 1) & (cx == 1)

    x_first = pltpu.make_async_copy(x.at[pl.ds(0, M)], xv.at[pl.ds(0, M)], xl_sem.at[0])
    x_last = pltpu.make_async_copy(x.at[pl.ds(M, rows - M)], xv.at[pl.ds(10 * M, rows - M)], xl_sem.at[1])
    tiles = half // TILE

    parts = len(FIRST)

    def w1_cols(side, start, width):
        return w1.at[:, pl.ds(pl.multiple_of(side * half + start, 128), width)]

    w1_send = [pltpu.make_async_copy(w1_cols(1 - cy, *piece), w1v.at[0, :, pl.ds(*piece)], w1_sem.at[k])
               for k, piece in enumerate(FIRST)]
    w1_keep = pltpu.make_async_copy(w1_cols(cy, 0, half), w1v.at[1], w1_sem.at[parts])
    width = w2.shape[1]

    def w2_rows(core, k):
        side = cy if k == 0 else 1 - cy
        return w2.at[pl.ds(pl.multiple_of((core * 2 + side) * half, half), half)]

    mine = pl.ds(pl.multiple_of(cx * width, width), width)
    w2_local = [pltpu.make_async_copy(w2_rows(cx, k), w2v.at[k, :, mine], w2_sem.at[k]) for k in range(2)]
    w2_swap = [remote(w2_rows(1 - cx, k), w2v.at[k, :, mine], bw_send.at[k], bw_recv.at[k], partner) for k in range(2)]
    x_swap = [
        remote(x.at[pl.ds(0, M)], xv.at[pl.ds(M, M)], bx_send.at[0], bx_recv.at[0], partner),
        remote(x.at[pl.ds(M, rows - M)], xv.at[pl.ds(8 * M, rows - M)], bx_send.at[1], bx_recv.at[1], partner),
    ]
    x_along = [remote(x.at[pl.ds(k * M, M)], xv.at[pl.ds((2 + k) * M, M)], xy_send.at[k], xy_recv.at[k], along)
               for k in range(per)]

    def x_forward(k):
        return remote(xv.at[at(2 + k)], xv.at[at(5 + k)], xf_send.at[k], xf_recv.at[k], partner)

    def p_copy(i):
        return remote(ps.at[at(i)], pr.at[at(i)], p_send.at[i], p_recv.at[i], across)

    def h_copy(i):
        return remote(ho.at[at(i)], hr.at[at(i)], h_send.at[i], h_recv.at[i], across)

    def z_copy(i, slot, row, device):
        return remote(zs.at[at(i)], zr.at[slot, at(row)], z_send.at[i], z_recv.at[i], device)

    def p_piece(k):
        c = pl.ds(*FIRST[k])
        sem = k if k == 0 else chunks - 1 + k
        return remote(ps.at[pl.ds(0, M), c], pr.at[pl.ds(0, M), c], p_send.at[sem], p_recv.at[sem], across)

    straight = half - DETOUR

    def p_last():
        c = pl.ds(0, straight)
        return remote(ps.at[at(last), c], pr.at[at(last), c], p_send.at[last], p_recv.at[last], across)

    detour = [
        remote(ra, rb, r_send.at[0], r_recv.at[0], diagonal),
        remote(rb, rc, r_send.at[1], r_recv.at[1], across),
        remote(rc, pr.at[at(last), pl.ds(straight, DETOUR)], r_send.at[2], r_recv.at[2], diagonal),
    ]

    def h_piece(k):
        c = pl.ds(*PIECES[k])
        return remote(ho.at[at(chunks - 1), c], hr.at[at(chunks - 1), c],
                      h_send.at[chunks - 1 + k], h_recv.at[chunks - 1 + k], across)

    barrier = pltpu.get_barrier_semaphore()
    for device in (across, partner, along, diagonal):
        pl.semaphore_signal(barrier, inc=1, device_id=device, device_id_type=MESH)

    x_first.start()
    w1_send[0].start()
    x_first.wait()
    for k in range(parts):
        c = pl.ds(*FIRST[k])
        w1_send[k].wait()
        if k == 0:
            w1_send[1].start()
        if k < parts - 2:
            w1_send[k + 2].start()
        ps[pl.ds(0, M), c] = jnp.dot(xv[pl.ds(0, M), :], w1v[0, :, c], preferred_element_type=F32)
        if k == 0:
            pl.semaphore_wait(barrier, 4)
        p_piece(k).start()

    x_last.start()
    w1_keep.start()
    for copy in w2_local:
        copy.start()
    x_swap[0].start()
    for copy in x_along:
        copy.start()
    x_swap[1].start()
    for copy in w2_swap:
        copy.start()
    x_last.wait()
    w1_keep.wait()

    def first_layer(i, side, out, out_rows):
        for n in range(half // TILE):
            c = pl.ds(n * TILE, TILE)
            out[out_rows, c] = jnp.dot(xv[at(i), :], w1v[side, :, c], preferred_element_type=F32)

    def partial(i):
        @pl.when(i == 1)
        def _():
            x_swap[0].wait_recv()

        @pl.when((i >= 2) & (i < 5))
        def _():
            k = i - 2
            remote(xv.at[at(i)], xv.at[at(i)], xy_send.at[k], xy_recv.at[k], along).wait_recv()
            x_forward(k).start()

        @pl.when((i >= 5) & (i < 8))
        def _():
            x_forward(i - 5).wait_recv()

        @pl.when(i == 8)
        def _():
            x_swap[1].wait_recv()

        first_layer(i, 0, ps, at(i))

        @pl.when(detours & (i == last))
        def _():
            p_last().start()

        @pl.when(~(detours & (i == last)))
        def _():
            p_copy(i).start()

    def activate(i, c):
        total = (po[:, c] + pr[at(i), c]).astype(BF16).astype(F32)
        ho[at(i), c] = gelu_tanh(total).astype(BF16)

    def hidden(i):
        first_layer(i, 1, po, pl.ds(0, M))

        @pl.when(i == 0)
        def _():
            for k in range(parts):
                p_piece(k).wait_recv()

        @pl.when(i > 0)
        def _():
            p_copy(i).wait_recv()

        for n in range(tiles):
            activate(i, pl.ds(n * TILE, TILE))
        h_copy(i).start()

    def second_own(i):
        for n in range(tiles):
            c = pl.ds(n * TILE, TILE)
            zs[at(i), c] = jnp.dot(ho[at(i), :], w2v[0, :, c], preferred_element_type=F32)

    def second_other(i):
        h_copy(i).wait_recv()
        for n in range(tiles):
            c = pl.ds(n * TILE, TILE)
            zs[at(i), c] += jnp.dot(hr[at(i), :], w2v[1, :, c], preferred_element_type=F32)

    def second_layer(i):
        @pl.when(i == 0)
        def _():
            for copy in w2_local:
                copy.wait()
            for copy in w2_swap:
                copy.wait_recv()

        second_own(i)
        second_other(i)

        @pl.when(i == 1)
        def _():
            z_copy(i, 0, 0, partner).start()

        @pl.when((i >= 2) & (i < 5))
        def _():
            z_copy(i, 1, i - 2, along).start()

        @pl.when((i >= 5) & (i < 8))
        def _():
            z_copy(i, 2, i - 5, diagonal).start()

        @pl.when((i >= 8) & (i < 10))
        def _():
            z_copy(i, 0, i - 7, partner).start()

    def step(t, carry):
        @pl.when(detours & (t == 3))
        def _():
            ra[...] = jnp.dot(xv[at(last), :], w1v[0, :, pl.ds(straight, DETOUR)], preferred_element_type=F32)
            detour[0].start()

        @pl.when(relays & (t == 4))
        def _():
            detour[0].wait_recv()
            detour[1].start()

        @pl.when(relays & (t == 7))
        def _():
            detour[1].wait_recv()
            detour[2].start()

        @pl.when(t >= 2)
        def _():
            hidden(t - 2)

        @pl.when(t < chunks)
        def _():
            partial(t)

        @pl.when(t >= 3)
        def _():
            second_layer(t - 3)

        return carry

    lax.fori_loop(1, chunks + 1, step, 0)

    first_layer(last, 1, po, pl.ds(0, M))

    @pl.when(detours)
    def _():
        p_last().wait_recv()
        detour[2].wait_recv()

    @pl.when(~detours)
    def _():
        p_copy(last).wait_recv()

    for k, piece in enumerate(PIECES):
        activate(last, pl.ds(*piece))
        h_piece(k).start()
    second_own(last)
    second_own(last - 1)

    def others(r):
        came = ((1, 2, 5), (8, 3, 6), (9, 4, 7))[r]
        for slot, i in enumerate(came):
            z_copy(i, slot, r, (partner, along, diagonal)[slot]).wait_recv()
        row = pl.ds(r * M, M)
        return row, lambda c: zr[0, row, c] + zr[1, row, c] + zr[2, row, c]

    def finish(r, i):
        row, came = others(r)
        for n in range(tiles):
            c = pl.ds(n * TILE, TILE)
            z[row, c] = (zs[at(i), c] + came(c)).astype(BF16)

    finish(0, 0)
    row, came = others(2)
    for n in range(tiles):
        c = pl.ds(n * TILE, TILE)
        zs[at(last), c] += came(c)
    second_other(last - 1)
    finish(1, last - 1)
    for k, (start, width) in enumerate(PIECES):
        h_piece(k).wait_recv()
        for n in range(tiles):
            c = pl.ds(n * TILE, TILE)
            total = zs[at(last), c] + jnp.dot(
                hr[at(last), pl.ds(start, width)], w2v[1, pl.ds(start, width), c], preferred_element_type=F32)
            if k < len(PIECES) - 1:
                zs[at(last), c] = total
            else:
                z[row, c] = total.astype(BF16)

    for copy in x_along + x_swap + w2_swap:
        copy.wait_send()
    for k in range(per):
        x_forward(k).wait_send()
    for k in range(parts):
        p_piece(k).wait_send()
    for i in range(1, last):
        p_copy(i).wait_send()

    @pl.when(detours)
    def _():
        p_last().wait_send()
        detour[0].wait_send()

    @pl.when(~detours)
    def _():
        p_copy(last).wait_send()

    @pl.when(relays)
    def _():
        detour[1].wait_send()
        detour[2].wait_send()

    for i in range(chunks - 1):
        h_copy(i).wait_send()
    for k in range(len(PIECES)):
        h_piece(k).wait_send()
    for i in range(1, 10):
        z_copy(i, 0, 0, partner).wait_send()


def solution(mesh):
    def body(x, w1, w2):
        rows, half = x.shape
        total, chunks = 4 * rows, 4 * rows // M
        dma = lambda n: pltpu.SemaphoreType.DMA((n,))
        first, last = chunks - 1 + len(FIRST), chunks - 1 + len(PIECES)
        return pl.pallas_call(
            kernel,
            out_shape=jax.ShapeDtypeStruct((rows, half), BF16),
            in_specs=[pl.BlockSpec(memory_space=pl.ANY)] * 3,
            out_specs=pl.BlockSpec(memory_space=pltpu.VMEM),
            scratch_shapes=[
                pltpu.VMEM((total, half), BF16),
                pltpu.VMEM((2, half, half), BF16),
                pltpu.VMEM((2, half, half), BF16),
                pltpu.VMEM((total, half), F32),
                pltpu.VMEM((total, half), F32),
                pltpu.VMEM((M, half), F32),
                pltpu.VMEM((total, half), BF16),
                pltpu.VMEM((total, half), BF16),
                pltpu.VMEM((total, half), F32),
                pltpu.VMEM((3, rows, half), F32),
                pltpu.VMEM((M, DETOUR), F32),
                pltpu.VMEM((M, DETOUR), F32),
                pltpu.VMEM((M, DETOUR), F32),
                dma(2), dma(len(FIRST) + 1), dma(2),
                dma(2), dma(2), dma(2), dma(2),
                dma(3), dma(3), dma(3), dma(3),
                dma(first), dma(first), dma(last), dma(last), dma(chunks), dma(chunks),
                dma(3), dma(3),
            ],
            compiler_params=pltpu.CompilerParams(
                collective_id=0, has_side_effects=True, vmem_limit_bytes=48 * 1024 * 1024
            ),
        )(pltpu.with_memory_space_constraint(x, pltpu.HBM), w1, w2)

    return jax.shard_map(
        body,
        mesh=mesh,
        in_specs=(P(("cx", "cz"), "cy"), P("cy", ("cz", "cx")), P("cz", ("cy", "cx"))),
        out_specs=P(("cx", "cz"), "cy"),
        check_vma=False,
    )
```

```python
import math

import jax
import jax.numpy as jnp
from jax import lax
from jax.experimental import pallas as pl
from jax.experimental.pallas import tpu as pltpu
from jax.sharding import PartitionSpec as P

MESH = pl.DeviceIdType.MESH
F32 = jnp.float32
BF16 = jnp.bfloat16
M = 64
TILE = 512
FIRST = ((0, 256), (256, 256), (512, 512), (1024, 512))
PIECES = ((0, 768), (768, 512), (1280, 256))
SLOTS = 4
DETOUR = 256


def gelu_tanh(c):
    return 0.5 * c * (1.0 + jnp.tanh(math.sqrt(2 / math.pi) * (c + 0.044715 * (c * c * c))))


def kernel(x, w1, w2, z, xv, w1v, w2v, ps, pr, po, ho, hr, zs, zr, ra, rb, rc,
           xl_sem, w1_sem, w2_sem, bx_send, bx_recv, bw_send, bw_recv,
           xy_send, xy_recv, xf_send, xf_recv, p_send, p_recv, h_send, h_recv, z_send, z_recv, r_send, r_recv):
    cz, cy, cx = lax.axis_index("cz"), lax.axis_index("cy"), lax.axis_index("cx")
    across = {"cy": 1 - cy}
    partner = {"cx": 1 - cx}
    along = {"cz": 1 - cz}
    diagonal = {"cz": 1 - cz, "cx": 1 - cx}
    rows, half = x.shape
    chunks = 4 * rows // M
    per = rows // M

    def remote(src, dst, send, recv, device):
        return pltpu.make_async_remote_copy(src_ref=src, dst_ref=dst, send_sem=send, recv_sem=recv,
                                            device_id=device, device_id_type=MESH)

    def at(i, n=M):
        return pl.ds(pl.multiple_of(i * M, M), n)

    last = chunks - 1
    detours = (cz == 0) & (cx == 0)
    relays = (cz == 1) & (cx == 1)

    x_first = pltpu.make_async_copy(x.at[pl.ds(0, M)], xv.at[pl.ds(0, M)], xl_sem.at[0])
    x_last = pltpu.make_async_copy(x.at[pl.ds(M, rows - M)], xv.at[pl.ds(10 * M, rows - M)], xl_sem.at[0])
    tiles = half // TILE

    def w1_cols(side, start, width):
        return w1.at[:, pl.ds(pl.multiple_of(side * half + start, 128), width)]

    w1_send = [pltpu.make_async_copy(w1_cols(1 - cy, *piece), w1v.at[0, :, pl.ds(*piece)], w1_sem.at[k % 2])
               for k, piece in enumerate(FIRST)]
    w1_keep = pltpu.make_async_copy(w1_cols(cy, 0, half), w1v.at[1], w1_sem.at[0])
    width = w2.shape[1]

    def w2_rows(core, k):
        side = cy if k == 0 else 1 - cy
        return w2.at[pl.ds(pl.multiple_of((core * 2 + side) * half, half), half)]

    mine = pl.ds(pl.multiple_of(cx * width, width), width)
    both = pl.ds(0, 2 * half)
    w2_half = [pl.ds(k * half, half) for k in range(2)]
    w2_local = [pltpu.make_async_copy(w2_rows(cx, k), w2v.at[w2_half[k], mine], w2_sem.at[0]) for k in range(2)]
    w2_local_all = pltpu.make_async_copy(w2.at[both], w2v.at[:, mine], w2_sem.at[0])
    w2_swap = [remote(w2_rows(1 - cx, k), w2v.at[w2_half[k], mine], bw_send.at[0], bw_recv.at[0], partner)
               for k in range(2)]
    w2_swap_all = remote(w2.at[both], w2v.at[:, mine], bw_send.at[0], bw_recv.at[0], partner)
    x_swap = [
        remote(x.at[pl.ds(0, M)], xv.at[pl.ds(M, M)], bx_send.at[0], bx_recv.at[0], partner),
        remote(x.at[pl.ds(M, rows - M)], xv.at[pl.ds(8 * M, rows - M)], bx_send.at[0], bx_recv.at[0], partner),
    ]
    x_swap_all = remote(x, xv.at[pl.ds(7 * M, rows)], bx_send.at[0], bx_recv.at[0], partner)
    x_along = [
        remote(x.at[pl.ds(0, M)], xv.at[pl.ds(2 * M, M)], xy_send.at[0], xy_recv.at[0], along),
        remote(x.at[pl.ds(M, rows - M)], xv.at[pl.ds(3 * M, rows - M)], xy_send.at[0], xy_recv.at[1], along),
    ]
    x_along_all = remote(x, xv.at[pl.ds(2 * M, rows)], xy_send.at[0], xy_recv.at[0], along)
    x_forward = [
        remote(xv.at[pl.ds(2 * M, M)], xv.at[pl.ds(5 * M, M)], xf_send.at[0], xf_recv.at[0], partner),
        remote(xv.at[pl.ds(3 * M, rows - M)], xv.at[pl.ds(6 * M, rows - M)], xf_send.at[0], xf_recv.at[0], partner),
    ]
    x_forward_all = remote(xv.at[pl.ds(2 * M, rows)], xv.at[pl.ds(5 * M, rows)], xf_send.at[0], xf_recv.at[0], partner)

    def p_copy(i):
        return remote(ps.at[at(i)], pr.at[at(i)], p_send.at[0], p_recv.at[i % SLOTS], across)

    def h_copy(i):
        return remote(ho.at[at(i)], hr.at[at(i)], h_send.at[0], h_recv.at[i % SLOTS], across)

    def z_copy(i, slot, row, device):
        return remote(zs.at[at(i)], zr.at[at(slot * per + row)], z_send.at[0], z_recv.at[0], device)

    z_all = remote(zs.at[pl.ds(0, 3 * rows)], zr, z_send.at[0], z_recv.at[0], partner)
    parts = len(FIRST)

    def p_piece(k):
        c = pl.ds(*FIRST[k])
        return remote(ps.at[pl.ds(0, M), c], pr.at[pl.ds(0, M), c], p_send.at[0], p_recv.at[0], across)

    straight = half - DETOUR

    def p_last():
        c = pl.ds(0, straight)
        return remote(ps.at[at(last), c], pr.at[at(last), c], p_send.at[1], p_recv.at[last % SLOTS], across)

    def p_whole():
        return remote(ps.at[at(last)], pr.at[at(last)], p_send.at[1], p_recv.at[last % SLOTS], across)

    detour = [
        remote(ra, rb, r_send.at[0], r_recv.at[0], diagonal),
        remote(rb, rc, r_send.at[0], r_recv.at[1], across),
        remote(rc, pr.at[at(last), pl.ds(straight, DETOUR)], r_send.at[0], r_recv.at[0], diagonal),
    ]

    def h_piece(k):
        c = pl.ds(*PIECES[k])
        return remote(ho.at[at(chunks - 1), c], hr.at[at(chunks - 1), c],
                      h_send.at[0], h_recv.at[SLOTS + k], across)

    barrier = pltpu.get_barrier_semaphore()
    for device in (across, partner, along, diagonal):
        pl.semaphore_signal(barrier, inc=1, device_id=device, device_id_type=MESH)

    x_first.start()
    w1_send[0].start()
    x_first.wait()
    for k in range(parts):
        c = pl.ds(*FIRST[k])
        w1_send[k].wait()
        if k == 0:
            w1_send[1].start()
        if k < parts - 2:
            w1_send[k + 2].start()
        ps[pl.ds(0, M), c] = jnp.dot(xv[pl.ds(0, M), :], w1v[0, :, c], preferred_element_type=F32)
        if k == 0:
            pl.semaphore_wait(barrier, 4)
        p_piece(k).start()

    x_last.start()
    w1_keep.start()
    for copy in w2_local:
        copy.start()
    x_swap[0].start()
    for copy in x_along:
        copy.start()
    x_swap[1].start()
    for copy in w2_swap:
        copy.start()
    x_last.wait()
    w1_keep.wait()

    def first_layer(i, side, out, out_rows):
        for n in range(half // TILE):
            c = pl.ds(n * TILE, TILE)
            out[out_rows, c] = jnp.dot(xv[at(i), :], w1v[side, :, c], preferred_element_type=F32)

    def partial(i):
        @pl.when(i == 1)
        def _():
            x_swap_all.wait_recv()

        for k in range(2):
            @pl.when(i == 2 + k)
            def _():
                x_along[k].wait_recv()
                x_forward[k].start()

        @pl.when(i == 5)
        def _():
            x_forward_all.wait_recv()

        first_layer(i, 0, ps, at(i))

        @pl.when(detours & (i == last))
        def _():
            p_last().start()

        @pl.when(~detours & (i == last))
        def _():
            p_whole().start()

        @pl.when(i < last)
        def _():
            p_copy(i).start()

    def activate(i, c):
        total = (po[:, c] + pr[at(i), c]).astype(BF16).astype(F32)
        ho[at(i), c] = gelu_tanh(total).astype(BF16)

    def hidden(i):
        first_layer(i, 1, po, pl.ds(0, M))
        p_copy(i).wait_recv()
        for n in range(tiles):
            activate(i, pl.ds(n * TILE, TILE))
        h_copy(i).start()

    def second_own(i):
        for n in range(tiles):
            c = pl.ds(n * TILE, TILE)
            zs[at(i), c] = jnp.dot(ho[at(i), :], w2v[w2_half[0], c], preferred_element_type=F32)

    def second_other(i):
        h_copy(i).wait_recv()
        for n in range(tiles):
            c = pl.ds(n * TILE, TILE)
            zs[at(i), c] += jnp.dot(hr[at(i), :], w2v[w2_half[1], c], preferred_element_type=F32)

    def second_layer(i):
        @pl.when(i == 0)
        def _():
            w2_local_all.wait()
            w2_swap_all.wait_recv()

        second_own(i)
        second_other(i)

        @pl.when(i == 1)
        def _():
            z_copy(i, 0, 0, partner).start()

        @pl.when((i >= 2) & (i < 5))
        def _():
            z_copy(i, 1, i - 2, along).start()

        @pl.when((i >= 5) & (i < 8))
        def _():
            z_copy(i, 2, i - 5, diagonal).start()

        @pl.when((i >= 8) & (i < 10))
        def _():
            z_copy(i, 0, i - 7, partner).start()

    def step(t, carry):
        @pl.when(detours & (t == 3))
        def _():
            ra[...] = jnp.dot(xv[at(last), :], w1v[0, :, pl.ds(straight, DETOUR)], preferred_element_type=F32)
            detour[0].start()

        @pl.when(relays & (t == 4))
        def _():
            detour[0].wait_recv()
            detour[1].start()

        @pl.when(relays & (t == 7))
        def _():
            detour[1].wait_recv()
            detour[1].wait_send()
            detour[2].start()

        @pl.when(t >= 2)
        def _():
            hidden(t - 2)

        @pl.when(t < chunks)
        def _():
            partial(t)

        @pl.when(t >= 3)
        def _():
            second_layer(t - 3)

        return carry

    lax.fori_loop(1, chunks + 1, step, 0)

    first_layer(last, 1, po, pl.ds(0, M))

    @pl.when(detours)
    def _():
        p_last().wait_recv()
        detour[2].wait_recv()

    @pl.when(~detours)
    def _():
        p_whole().wait_recv()

    for k, piece in enumerate(PIECES):
        activate(last, pl.ds(*piece))
        h_piece(k).start()
    second_own(last)
    second_own(last - 1)

    z_all.wait_recv()

    def came(r, c):
        return zr[pl.ds(r * M, M), c] + zr[pl.ds(rows + r * M, M), c] + zr[pl.ds(2 * rows + r * M, M), c]

    def finish(r, i):
        for n in range(tiles):
            c = pl.ds(n * TILE, TILE)
            z[pl.ds(r * M, M), c] = (zs[at(i), c] + came(r, c)).astype(BF16)

    finish(0, 0)
    for n in range(tiles):
        c = pl.ds(n * TILE, TILE)
        zs[at(last), c] += came(2, c)
    second_other(last - 1)
    finish(1, last - 1)
    for k, (start, width) in enumerate(PIECES):
        h_piece(k).wait_recv()
        for n in range(tiles):
            c = pl.ds(n * TILE, TILE)
            total = zs[at(last), c] + jnp.dot(
                hr[at(last), pl.ds(start, width)], w2v[pl.ds(half + start, width), c], preferred_element_type=F32)
            if k < len(PIECES) - 1:
                zs[at(last), c] = total
            else:
                z[pl.ds(2 * M, M), c] = total.astype(BF16)

    for copy in (x_along_all, x_swap_all, w2_swap_all, x_forward_all, z_all):
        copy.wait_send()
    most = pl.ds(0, last * M)
    remote(ps.at[most], pr.at[most], p_send.at[0], p_recv.at[0], across).wait_send()
    remote(ho, hr, h_send.at[0], h_recv.at[0], across).wait_send()

    @pl.when(detours)
    def _():
        p_last().wait_send()
        detour[0].wait_send()

    @pl.when(~detours)
    def _():
        p_whole().wait_send()

    @pl.when(relays)
    def _():
        detour[2].wait_send()


def solution(mesh):
    def body(x, w1, w2):
        rows, half = x.shape
        total = 4 * rows
        dma = lambda n: pltpu.SemaphoreType.DMA((n,))
        return pl.pallas_call(
            kernel,
            out_shape=jax.ShapeDtypeStruct((rows, half), BF16),
            in_specs=[pl.BlockSpec(memory_space=pl.ANY)] * 3,
            out_specs=pl.BlockSpec(memory_space=pltpu.VMEM),
            scratch_shapes=[
                pltpu.VMEM((total, half), BF16),
                pltpu.VMEM((2, half, half), BF16),
                pltpu.VMEM((2 * half, half), BF16),
                pltpu.VMEM((total, half), F32),
                pltpu.VMEM((total, half), F32),
                pltpu.VMEM((M, half), F32),
                pltpu.VMEM((total, half), BF16),
                pltpu.VMEM((total, half), BF16),
                pltpu.VMEM((total, half), F32),
                pltpu.VMEM((3 * rows, half), F32),
                pltpu.VMEM((M, DETOUR), F32),
                pltpu.VMEM((M, DETOUR), F32),
                pltpu.VMEM((M, DETOUR), F32),
                dma(1), dma(2), dma(1),
                dma(1), dma(1), dma(1), dma(1),
                dma(1), dma(2), dma(1), dma(1),
                dma(2), dma(SLOTS), dma(1), dma(SLOTS + len(PIECES)),
                dma(1), dma(1), dma(1), dma(2),
            ],
            compiler_params=pltpu.CompilerParams(
                collective_id=0, has_side_effects=True, vmem_limit_bytes=48 * 1024 * 1024
            ),
        )(pltpu.with_memory_space_constraint(x, pltpu.HBM), w1, w2)

    return jax.shard_map(
        body,
        mesh=mesh,
        in_specs=(P(("cx", "cz"), "cy"), P("cy", ("cz", "cx")), P("cz", ("cy", "cx"))),
        out_specs=P(("cx", "cz"), "cy"),
        check_vma=False,
    )
```

```python
import math

import jax
import jax.numpy as jnp
from jax import lax
from jax.experimental import pallas as pl
from jax.experimental.pallas import tpu as pltpu
from jax.sharding import PartitionSpec as P

MESH = pl.DeviceIdType.MESH
F32 = jnp.float32
BF16 = jnp.bfloat16
M = 64
TILE = 512
FIRST = ((0, 256), (256, 256), (512, 512), (1024, 512))
SKEW = 256
TO_LOW = ((0, 768), (768, 512), (1280, 256))
TO_HIGH = ((0, 768), (768, 256), (1024, 256))
SLOTS = 4
DETOUR = 256


def gelu_tanh(c):
    return 0.5 * c * (1.0 + jnp.tanh(math.sqrt(2 / math.pi) * (c + 0.044715 * (c * c * c))))


def kernel(x, w1, w2, z, xv, w1v, w2v, ps, pr, po, ho, hr, zs, zr, ra, rb, rc, pe, pq,
           xl_sem, w1_sem, w2_sem, bx_send, bx_recv, bw_send, bw_recv,
           xy_send, xy_recv, xf_send, xf_recv, p_send, p_recv, h_send, h_recv, z_send, z_recv, r_send, r_recv):
    cz, cy, cx = lax.axis_index("cz"), lax.axis_index("cy"), lax.axis_index("cx")
    across = {"cy": 1 - cy}
    partner = {"cx": 1 - cx}
    along = {"cz": 1 - cz}
    diagonal = {"cz": 1 - cz, "cx": 1 - cx}
    rows, half = x.shape
    chunks = 4 * rows // M
    per = rows // M

    def remote(src, dst, send, recv, device):
        return pltpu.make_async_remote_copy(src_ref=src, dst_ref=dst, send_sem=send, recv_sem=recv,
                                            device_id=device, device_id_type=MESH)

    def at(i, n=M):
        return pl.ds(pl.multiple_of(i * M, M), n)

    last = chunks - 1
    low, high = cy == 0, cy == 1
    kept = half - SKEW
    detours = (cz == 0) & (cx == 0)
    relays = (cz == 1) & (cx == 1)

    x_first = pltpu.make_async_copy(x.at[pl.ds(0, M)], xv.at[pl.ds(0, M)], xl_sem.at[0])
    x_last = pltpu.make_async_copy(x.at[pl.ds(M, rows - M)], xv.at[pl.ds(10 * M, rows - M)], xl_sem.at[0])
    tiles = half // TILE

    def w1_cols(side, start, width):
        return w1.at[:, pl.ds(pl.multiple_of(side * half + start, 128), width)]

    w1_send = [pltpu.make_async_copy(w1_cols(1 - cy, *piece), w1v.at[0, :, pl.ds(*piece)], w1_sem.at[k % 2])
               for k, piece in enumerate(FIRST)]
    w1_keep = pltpu.make_async_copy(w1_cols(cy, 0, half), w1v.at[1], w1_sem.at[0])
    width = w2.shape[1]

    def w2_rows(core, k):
        side = cy if k == 0 else 1 - cy
        return w2.at[pl.ds(pl.multiple_of((core * 2 + side) * half, half), half)]

    mine = pl.ds(pl.multiple_of(cx * width, width), width)
    both = pl.ds(0, 2 * half)
    w2_half = [pl.ds(k * half, half) for k in range(2)]
    w2_local = [pltpu.make_async_copy(w2_rows(cx, k), w2v.at[w2_half[k], mine], w2_sem.at[0]) for k in range(2)]
    w2_local_all = pltpu.make_async_copy(w2.at[both], w2v.at[:, mine], w2_sem.at[0])
    w2_swap = [remote(w2_rows(1 - cx, k), w2v.at[w2_half[k], mine], bw_send.at[0], bw_recv.at[0], partner)
               for k in range(2)]
    w2_swap_all = remote(w2.at[both], w2v.at[:, mine], bw_send.at[0], bw_recv.at[0], partner)
    x_swap = [
        remote(x.at[pl.ds(0, M)], xv.at[pl.ds(M, M)], bx_send.at[0], bx_recv.at[0], partner),
        remote(x.at[pl.ds(M, rows - M)], xv.at[pl.ds(8 * M, rows - M)], bx_send.at[0], bx_recv.at[0], partner),
    ]
    x_swap_all = remote(x, xv.at[pl.ds(7 * M, rows)], bx_send.at[0], bx_recv.at[0], partner)
    x_along = [
        remote(x.at[pl.ds(0, M)], xv.at[pl.ds(2 * M, M)], xy_send.at[0], xy_recv.at[0], along),
        remote(x.at[pl.ds(M, rows - M)], xv.at[pl.ds(3 * M, rows - M)], xy_send.at[0], xy_recv.at[1], along),
    ]
    x_along_all = remote(x, xv.at[pl.ds(2 * M, rows)], xy_send.at[0], xy_recv.at[0], along)
    x_forward = [
        remote(xv.at[pl.ds(2 * M, M)], xv.at[pl.ds(5 * M, M)], xf_send.at[0], xf_recv.at[0], partner),
        remote(xv.at[pl.ds(3 * M, rows - M)], xv.at[pl.ds(6 * M, rows - M)], xf_send.at[0], xf_recv.at[0], partner),
    ]
    x_forward_all = remote(xv.at[pl.ds(2 * M, rows)], xv.at[pl.ds(5 * M, rows)], xf_send.at[0], xf_recv.at[0], partner)

    def p_copy(i):
        return remote(ps.at[at(i)], pr.at[at(i)], p_send.at[0], p_recv.at[i % SLOTS], across)

    def h_copy(i):
        return remote(ho.at[at(i)], hr.at[at(i)], h_send.at[0], h_recv.at[i % SLOTS], across)

    def z_copy(i, slot, row, device):
        return remote(zs.at[at(i)], zr.at[at(slot * per + row)], z_send.at[0], z_recv.at[0], device)

    z_all = remote(zs.at[pl.ds(0, 3 * rows)], zr, z_send.at[0], z_recv.at[0], partner)
    parts = len(FIRST)

    def p_piece(k):
        c = pl.ds(*FIRST[k])
        return remote(ps.at[pl.ds(0, M), c], pr.at[pl.ds(0, M), c], p_send.at[0], p_recv.at[0], across)

    straight = half - DETOUR

    def p_straight():
        c = pl.ds(0, straight)
        return remote(ps.at[at(last - 1), c], pr.at[at(last - 1), c], p_send.at[1], p_recv.at[(last - 1) % SLOTS], across)

    def p_whole():
        return remote(ps.at[at(last - 1)], pr.at[at(last - 1)], p_send.at[1], p_recv.at[(last - 1) % SLOTS], across)

    def p_high():
        return remote(ps.at[at(last)], pr.at[at(last)], p_send.at[2], p_recv.at[last % SLOTS], across)

    def p_over():
        return remote(pe, pq, p_send.at[3], p_recv.at[SLOTS], across)

    def p_low():
        c = pl.ds(0, kept)
        return remote(ps.at[at(last), c], pr.at[at(last), c], p_send.at[2], p_recv.at[last % SLOTS], across)

    detour = [
        remote(ra, rb, r_send.at[0], r_recv.at[0], diagonal),
        remote(rb, rc, r_send.at[0], r_recv.at[1], across),
        remote(rc, pr.at[at(last - 1), pl.ds(straight, DETOUR)], r_send.at[0], r_recv.at[0], diagonal),
    ]

    def h_piece(k, piece):
        c = pl.ds(*piece)
        return remote(ho.at[at(last), c], hr.at[at(last), c], h_send.at[1], h_recv.at[SLOTS + k], across)

    def h_over():
        c = pl.ds(kept, SKEW)
        return remote(hr.at[at(last), c], ho.at[at(last), c], h_send.at[2], h_recv.at[SLOTS + len(TO_LOW)], across)

    barrier = pltpu.get_barrier_semaphore()
    for device in (across, partner, along, diagonal):
        pl.semaphore_signal(barrier, inc=1, device_id=device, device_id_type=MESH)

    x_first.start()
    w1_send[0].start()
    x_first.wait()
    for k in range(parts):
        c = pl.ds(*FIRST[k])
        w1_send[k].wait()
        if k == 0:
            w1_send[1].start()
        if k < parts - 2:
            w1_send[k + 2].start()
        ps[pl.ds(0, M), c] = jnp.dot(xv[pl.ds(0, M), :], w1v[0, :, c], preferred_element_type=F32)
        if k == 0:
            pl.semaphore_wait(barrier, 4)
        p_piece(k).start()

    x_last.start()
    w1_keep.start()
    for copy in w2_local:
        copy.start()
    x_swap[0].start()
    for copy in x_along:
        copy.start()
    x_swap[1].start()
    for copy in w2_swap:
        copy.start()
    x_last.wait()
    w1_keep.wait()

    def first_layer(i, side, out, out_rows):
        for n in range(half // TILE):
            c = pl.ds(n * TILE, TILE)
            out[out_rows, c] = jnp.dot(xv[at(i), :], w1v[side, :, c], preferred_element_type=F32)

    def partial(i):
        @pl.when(i == 1)
        def _():
            x_swap_all.wait_recv()

        for k in range(2):
            @pl.when(i == 2 + k)
            def _():
                x_along[k].wait_recv()
                x_forward[k].start()

        @pl.when(i == 5)
        def _():
            x_forward_all.wait_recv()

        @pl.when(low & (i == last))
        def _():
            pe[...] = jnp.dot(xv[at(last), :], w1v[1, :, pl.ds(kept, SKEW)], preferred_element_type=F32)
            p_over().start()

        first_layer(i, 0, ps, at(i))

        @pl.when(i < last - 1)
        def _():
            p_copy(i).start()

        @pl.when(detours & (i == last - 1))
        def _():
            p_straight().start()

        @pl.when(~detours & (i == last - 1))
        def _():
            p_whole().start()

        @pl.when(low & (i == last))
        def _():
            p_high().start()

        @pl.when(high & (i == last))
        def _():
            p_low().start()

    def activate(i, c):
        total = (po[:, c] + pr[at(i), c]).astype(BF16).astype(F32)
        ho[at(i), c] = gelu_tanh(total).astype(BF16)

    def hidden(i):
        first_layer(i, 1, po, pl.ds(0, M))

        @pl.when(~detours | (i < last - 1))
        def _():
            p_copy(i).wait_recv()

        @pl.when(detours & (i == last - 1))
        def _():
            p_straight().wait_recv()
            detour[2].wait_recv()

        for n in range(tiles):
            activate(i, pl.ds(n * TILE, TILE))
        h_copy(i).start()

    def second_own(i):
        for n in range(tiles):
            c = pl.ds(n * TILE, TILE)
            zs[at(i), c] = jnp.dot(ho[at(i), :], w2v[w2_half[0], c], preferred_element_type=F32)

    def second_other(i):
        h_copy(i).wait_recv()
        for n in range(tiles):
            c = pl.ds(n * TILE, TILE)
            zs[at(i), c] += jnp.dot(hr[at(i), :], w2v[w2_half[1], c], preferred_element_type=F32)

    def second_layer(i):
        @pl.when(i == 0)
        def _():
            w2_local_all.wait()
            w2_swap_all.wait_recv()

        second_own(i)
        second_other(i)

        @pl.when(i == 1)
        def _():
            z_copy(i, 0, 0, partner).start()

        @pl.when((i >= 2) & (i < 5))
        def _():
            z_copy(i, 1, i - 2, along).start()

        @pl.when((i >= 5) & (i < 8))
        def _():
            z_copy(i, 2, i - 5, diagonal).start()

        @pl.when((i >= 8) & (i < 10))
        def _():
            z_copy(i, 0, i - 7, partner).start()

    def step(t, carry):
        @pl.when(detours & (t == 3))
        def _():
            ra[...] = jnp.dot(xv[at(last - 1), :], w1v[0, :, pl.ds(straight, DETOUR)], preferred_element_type=F32)
            detour[0].start()

        @pl.when(relays & (t == 4))
        def _():
            detour[0].wait_recv()
            detour[1].start()

        @pl.when(relays & (t == 7))
        def _():
            detour[1].wait_recv()
            detour[1].wait_send()
            detour[2].start()

        @pl.when(t >= 2)
        def _():
            hidden(t - 2)

        @pl.when(t < chunks)
        def _():
            partial(t)

        @pl.when(t >= 3)
        def _():
            second_layer(t - 3)

        return carry

    lax.fori_loop(1, chunks + 1, step, 0)

    first_layer(last, 1, po, pl.ds(0, M))

    @pl.when(low)
    def _():
        p_low().wait_recv()
        for k, piece in enumerate(TO_HIGH):
            activate(last, pl.ds(*piece))
            h_piece(k, piece).start()

    over = pl.ds(kept, SKEW)

    @pl.when(high)
    def _():
        p_over().wait_recv()
        total = (ps[at(last), over] + pq[...]).astype(BF16).astype(F32)
        hr[at(last), over] = gelu_tanh(total).astype(BF16)
        h_over().start()
        p_high().wait_recv()
        for k, piece in enumerate(TO_LOW):
            activate(last, pl.ds(*piece))
            h_piece(k, piece).start()

    def multiply(h, start, width, below, out):
        for n in range(tiles):
            c = pl.ds(n * TILE, TILE)
            out(c, jnp.dot(h[at(last), pl.ds(start, width)], w2v[pl.ds(below + start, width), c],
                           preferred_element_type=F32))

    def put(c, term):
        zs[at(last), c] = term

    def add(c, term):
        zs[at(last), c] += term

    def close(c, term):
        z[pl.ds(2 * M, M), c] = (zs[at(last), c] + term).astype(BF16)

    multiply(ho, 0, kept, 0, put)

    @pl.when(high)
    def _():
        multiply(ho, kept, SKEW, 0, add)
        multiply(hr, kept, SKEW, half, add)

    second_own(last - 1)

    z_all.wait_recv()

    def came(r, c):
        return zr[pl.ds(r * M, M), c] + zr[pl.ds(rows + r * M, M), c] + zr[pl.ds(2 * rows + r * M, M), c]

    def finish(r, i):
        for n in range(tiles):
            c = pl.ds(n * TILE, TILE)
            z[pl.ds(r * M, M), c] = (zs[at(i), c] + came(r, c)).astype(BF16)

    finish(0, 0)
    for n in range(tiles):
        c = pl.ds(n * TILE, TILE)
        zs[at(last), c] += came(2, c)
    second_other(last - 1)
    finish(1, last - 1)

    def close_pieces(pieces):
        for k, piece in enumerate(pieces):
            h_piece(k, piece).wait_recv()
            multiply(hr, *piece, half, add if k < len(pieces) - 1 else close)

    @pl.when(low)
    def _():
        h_over().wait_recv()
        multiply(ho, kept, SKEW, 0, add)
        close_pieces(TO_LOW)

    @pl.when(high)
    def _():
        close_pieces(TO_HIGH)

    for copy in (x_along_all, x_swap_all, w2_swap_all, x_forward_all, z_all):
        copy.wait_send()
    most = pl.ds(0, (last - 1) * M)
    remote(ps.at[most], pr.at[most], p_send.at[0], p_recv.at[0], across).wait_send()
    most = pl.ds(0, last * M)
    remote(ho.at[most], hr.at[most], h_send.at[0], h_recv.at[0], across).wait_send()

    @pl.when(detours)
    def _():
        p_straight().wait_send()
        detour[0].wait_send()

    @pl.when(~detours)
    def _():
        p_whole().wait_send()

    @pl.when(low)
    def _():
        p_high().wait_send()
        p_over().wait_send()
        h_piece(0, (0, kept)).wait_send()

    @pl.when(high)
    def _():
        p_low().wait_send()
        h_over().wait_send()
        h_piece(0, (0, half)).wait_send()

    @pl.when(relays)
    def _():
        detour[2].wait_send()


def solution(mesh):
    def body(x, w1, w2):
        rows, half = x.shape
        total = 4 * rows
        dma = lambda n: pltpu.SemaphoreType.DMA((n,))
        return pl.pallas_call(
            kernel,
            out_shape=jax.ShapeDtypeStruct((rows, half), BF16),
            in_specs=[pl.BlockSpec(memory_space=pl.ANY)] * 3,
            out_specs=pl.BlockSpec(memory_space=pltpu.VMEM),
            scratch_shapes=[
                pltpu.VMEM((total, half), BF16),
                pltpu.VMEM((2, half, half), BF16),
                pltpu.VMEM((2 * half, half), BF16),
                pltpu.VMEM((total, half), F32),
                pltpu.VMEM((total, half), F32),
                pltpu.VMEM((M, half), F32),
                pltpu.VMEM((total, half), BF16),
                pltpu.VMEM((total, half), BF16),
                pltpu.VMEM((total, half), F32),
                pltpu.VMEM((3 * rows, half), F32),
                pltpu.VMEM((M, DETOUR), F32),
                pltpu.VMEM((M, DETOUR), F32),
                pltpu.VMEM((M, DETOUR), F32),
                pltpu.VMEM((M, SKEW), F32),
                pltpu.VMEM((M, SKEW), F32),
                dma(1), dma(2), dma(1),
                dma(1), dma(1), dma(1), dma(1),
                dma(1), dma(2), dma(1), dma(1),
                dma(4), dma(SLOTS + 1), dma(3), dma(SLOTS + len(TO_LOW) + 1),
                dma(1), dma(1), dma(1), dma(2),
            ],
            compiler_params=pltpu.CompilerParams(
                collective_id=0, has_side_effects=True, vmem_limit_bytes=48 * 1024 * 1024
            ),
        )(pltpu.with_memory_space_constraint(x, pltpu.HBM), w1, w2)

    return jax.shard_map(
        body,
        mesh=mesh,
        in_specs=(P(("cx", "cz"), "cy"), P("cy", ("cz", "cx")), P("cz", ("cy", "cx"))),
        out_specs=P(("cx", "cz"), "cy"),
        check_vma=False,
    )
```

```python
import math

import jax
import jax.numpy as jnp
from jax import lax
from jax.experimental import pallas as pl
from jax.experimental.pallas import tpu as pltpu
from jax.sharding import PartitionSpec as P

MESH = pl.DeviceIdType.MESH
F32 = jnp.float32
BF16 = jnp.bfloat16
M = 64
TILE = 512
FIRST = ((0, 256), (256, 256), (512, 512), (1024, 512))
SKEW = 256
TO_LOW = ((0, 768), (768, 512), (1280, 256))
TO_HIGH = ((0, 768), (768, 256), (1024, 256))
SLOTS = 4
DETOUR = 256


def gelu_tanh(c):
    return 0.5 * c * (1.0 + jnp.tanh(math.sqrt(2 / math.pi) * (c + 0.044715 * (c * c * c))))


def kernel(x, w1, w2, z, xv, w1v, w2v, ps, pr, po, ho, hr, zs, zr, ra, rb, rc, pe, pq,
           xl_sem, w1_sem, w2_sem, bx_send, bx_recv, bw_send, bw_recv,
           xy_send, xy_recv, xf_send, xf_recv, p_send, p_recv, h_send, h_recv, z_send, z_recv, r_send, r_recv):
    cz, cy, cx = lax.axis_index("cz"), lax.axis_index("cy"), lax.axis_index("cx")
    across = {"cy": 1 - cy}
    partner = {"cx": 1 - cx}
    along = {"cz": 1 - cz}
    diagonal = {"cz": 1 - cz, "cx": 1 - cx}
    rows, half = x.shape
    chunks = 4 * rows // M
    per = rows // M

    def remote(src, dst, send, recv, device):
        return pltpu.make_async_remote_copy(src_ref=src, dst_ref=dst, send_sem=send, recv_sem=recv,
                                            device_id=device, device_id_type=MESH)

    def at(i, n=M):
        return pl.ds(pl.multiple_of(i * M, M), n)

    last = chunks - 1
    low, high = cy == 0, cy == 1
    kept = half - SKEW
    source, sink = (cz == 0) & (cx == 0) & high, (cz == 0) & (cx == 0) & low
    relay_high, relay_low = (cz == 1) & (cx == 0) & high, (cz == 1) & (cx == 0) & low

    x_first = pltpu.make_async_copy(x.at[pl.ds(0, M)], xv.at[pl.ds(0, M)], xl_sem.at[0])
    x_last = pltpu.make_async_copy(x.at[pl.ds(M, rows - M)], xv.at[pl.ds(10 * M, rows - M)], xl_sem.at[0])
    tiles = half // TILE

    def w1_cols(side, start, width):
        return w1.at[:, pl.ds(pl.multiple_of(side * half + start, 128), width)]

    w1_send = [pltpu.make_async_copy(w1_cols(1 - cy, *piece), w1v.at[0, :, pl.ds(*piece)], w1_sem.at[k % 2])
               for k, piece in enumerate(FIRST)]
    w1_keep = pltpu.make_async_copy(w1_cols(cy, 0, half), w1v.at[1], w1_sem.at[0])
    width = w2.shape[1]

    def w2_rows(core, k):
        side = cy if k == 0 else 1 - cy
        return w2.at[pl.ds(pl.multiple_of((core * 2 + side) * half, half), half)]

    mine = pl.ds(pl.multiple_of(cx * width, width), width)
    both = pl.ds(0, 2 * half)
    w2_half = [pl.ds(k * half, half) for k in range(2)]
    w2_local = [pltpu.make_async_copy(w2_rows(cx, k), w2v.at[w2_half[k], mine], w2_sem.at[0]) for k in range(2)]
    w2_local_all = pltpu.make_async_copy(w2.at[both], w2v.at[:, mine], w2_sem.at[0])
    w2_swap = [remote(w2_rows(1 - cx, k), w2v.at[w2_half[k], mine], bw_send.at[0], bw_recv.at[0], partner)
               for k in range(2)]
    w2_swap_all = remote(w2.at[both], w2v.at[:, mine], bw_send.at[0], bw_recv.at[0], partner)
    x_swap = [
        remote(x.at[pl.ds(0, M)], xv.at[pl.ds(M, M)], bx_send.at[0], bx_recv.at[0], partner),
        remote(x.at[pl.ds(M, rows - M)], xv.at[pl.ds(8 * M, rows - M)], bx_send.at[0], bx_recv.at[0], partner),
    ]
    x_swap_all = remote(x, xv.at[pl.ds(7 * M, rows)], bx_send.at[0], bx_recv.at[0], partner)
    x_along = [
        remote(x.at[pl.ds(0, M)], xv.at[pl.ds(2 * M, M)], xy_send.at[0], xy_recv.at[0], along),
        remote(x.at[pl.ds(M, rows - M)], xv.at[pl.ds(3 * M, rows - M)], xy_send.at[0], xy_recv.at[1], along),
    ]
    x_along_all = remote(x, xv.at[pl.ds(2 * M, rows)], xy_send.at[0], xy_recv.at[0], along)
    x_forward = [
        remote(xv.at[pl.ds(2 * M, M)], xv.at[pl.ds(5 * M, M)], xf_send.at[0], xf_recv.at[0], partner),
        remote(xv.at[pl.ds(3 * M, rows - M)], xv.at[pl.ds(6 * M, rows - M)], xf_send.at[0], xf_recv.at[0], partner),
    ]
    x_forward_all = remote(xv.at[pl.ds(2 * M, rows)], xv.at[pl.ds(5 * M, rows)], xf_send.at[0], xf_recv.at[0], partner)

    def p_copy(i):
        return remote(ps.at[at(i)], pr.at[at(i)], p_send.at[0], p_recv.at[i % SLOTS], across)

    def h_copy(i):
        return remote(ho.at[at(i)], hr.at[at(i)], h_send.at[0], h_recv.at[i % SLOTS], across)

    def z_copy(i, slot, row, device):
        return remote(zs.at[at(i)], zr.at[at(slot * per + row)], z_send.at[0], z_recv.at[0], device)

    z_all = remote(zs.at[pl.ds(0, 3 * rows)], zr, z_send.at[0], z_recv.at[0], partner)
    parts = len(FIRST)

    def p_piece(k):
        c = pl.ds(*FIRST[k])
        return remote(ps.at[pl.ds(0, M), c], pr.at[pl.ds(0, M), c], p_send.at[0], p_recv.at[0], across)

    straight = half - DETOUR

    def p_straight():
        c = pl.ds(0, straight)
        return remote(ps.at[at(last - 1), c], pr.at[at(last - 1), c], p_send.at[1], p_recv.at[(last - 1) % SLOTS], across)

    def p_whole():
        return remote(ps.at[at(last - 1)], pr.at[at(last - 1)], p_send.at[1], p_recv.at[(last - 1) % SLOTS], across)

    def p_high():
        return remote(ps.at[at(last)], pr.at[at(last)], p_send.at[2], p_recv.at[last % SLOTS], across)

    def p_over():
        return remote(pe, pq, p_send.at[3], p_recv.at[SLOTS], across)

    def p_low():
        c = pl.ds(0, kept)
        return remote(ps.at[at(last), c], pr.at[at(last), c], p_send.at[2], p_recv.at[last % SLOTS], across)

    detour = [
        remote(ra, rb, r_send.at[0], r_recv.at[0], along),
        remote(rb, rc, r_send.at[0], r_recv.at[0], across),
        remote(rc, pr.at[at(last - 1), pl.ds(straight, DETOUR)], r_send.at[0], r_recv.at[0], along),
    ]

    def h_piece(k, piece):
        c = pl.ds(*piece)
        return remote(ho.at[at(last), c], hr.at[at(last), c], h_send.at[1], h_recv.at[SLOTS + k], across)

    def h_over():
        c = pl.ds(kept, SKEW)
        return remote(hr.at[at(last), c], ho.at[at(last), c], h_send.at[2], h_recv.at[SLOTS + len(TO_LOW)], across)

    barrier = pltpu.get_barrier_semaphore()
    for device in (across, partner, along, diagonal):
        pl.semaphore_signal(barrier, inc=1, device_id=device, device_id_type=MESH)

    x_first.start()
    w1_send[0].start()
    x_first.wait()
    for k in range(parts):
        c = pl.ds(*FIRST[k])
        w1_send[k].wait()
        if k == 0:
            w1_send[1].start()
        if k < parts - 2:
            w1_send[k + 2].start()
        ps[pl.ds(0, M), c] = jnp.dot(xv[pl.ds(0, M), :], w1v[0, :, c], preferred_element_type=F32)
        if k == 0:
            pl.semaphore_wait(barrier, 4)
        p_piece(k).start()

    x_last.start()
    w1_keep.start()
    for copy in w2_local:
        copy.start()
    x_swap[0].start()
    for copy in x_along:
        copy.start()
    x_swap[1].start()
    for copy in w2_swap:
        copy.start()
    x_last.wait()
    w1_keep.wait()

    def first_layer(i, side, out, out_rows):
        for n in range(half // TILE):
            c = pl.ds(n * TILE, TILE)
            out[out_rows, c] = jnp.dot(xv[at(i), :], w1v[side, :, c], preferred_element_type=F32)

    def partial(i):
        @pl.when(i == 1)
        def _():
            x_swap_all.wait_recv()

        for k in range(2):
            @pl.when(i == 2 + k)
            def _():
                x_along[k].wait_recv()
                x_forward[k].start()

        @pl.when(i == 5)
        def _():
            x_forward_all.wait_recv()

        @pl.when(low & (i == last))
        def _():
            pe[...] = jnp.dot(xv[at(last), :], w1v[1, :, pl.ds(kept, SKEW)], preferred_element_type=F32)
            p_over().start()

        first_layer(i, 0, ps, at(i))

        @pl.when(i < last - 1)
        def _():
            p_copy(i).start()

        @pl.when(source & (i == last - 1))
        def _():
            p_straight().start()

        @pl.when(~source & (i == last - 1))
        def _():
            p_whole().start()

        @pl.when(low & (i == last))
        def _():
            p_high().start()

        @pl.when(high & (i == last))
        def _():
            p_low().start()

    def activate(i, c):
        total = (po[:, c] + pr[at(i), c]).astype(BF16).astype(F32)
        ho[at(i), c] = gelu_tanh(total).astype(BF16)

    def hidden(i):
        first_layer(i, 1, po, pl.ds(0, M))

        @pl.when(~sink | (i < last - 1))
        def _():
            p_copy(i).wait_recv()

        @pl.when(sink & (i == last - 1))
        def _():
            p_straight().wait_recv()
            detour[2].wait_recv()

        for n in range(tiles):
            activate(i, pl.ds(n * TILE, TILE))
        h_copy(i).start()

    def second_own(i):
        for n in range(tiles):
            c = pl.ds(n * TILE, TILE)
            zs[at(i), c] = jnp.dot(ho[at(i), :], w2v[w2_half[0], c], preferred_element_type=F32)

    def second_other(i):
        h_copy(i).wait_recv()
        for n in range(tiles):
            c = pl.ds(n * TILE, TILE)
            zs[at(i), c] += jnp.dot(hr[at(i), :], w2v[w2_half[1], c], preferred_element_type=F32)

    def second_layer(i):
        second_other(i)

        @pl.when(i == 1)
        def _():
            z_copy(i, 0, 0, partner).start()

        @pl.when((i >= 2) & (i < 5))
        def _():
            z_copy(i, 1, i - 2, along).start()

        @pl.when((i >= 5) & (i < 8))
        def _():
            z_copy(i, 2, i - 5, diagonal).start()

        @pl.when((i >= 8) & (i < 10))
        def _():
            z_copy(i, 0, i - 7, partner).start()

    def multiply(h, start, width, below, out):
        for n in range(tiles):
            c = pl.ds(n * TILE, TILE)
            out(c, jnp.dot(h[at(last), pl.ds(start, width)], w2v[pl.ds(below + start, width), c],
                           preferred_element_type=F32))

    def put(c, term):
        zs[at(last), c] = term

    def add(c, term):
        zs[at(last), c] += term

    over = pl.ds(kept, SKEW)

    def hidden_last():
        first_layer(last, 1, po, pl.ds(0, M))

        @pl.when(low)
        def _():
            p_low().wait_recv()
            for k, piece in enumerate(TO_HIGH):
                activate(last, pl.ds(*piece))
                h_piece(k, piece).start()

        @pl.when(high)
        def _():
            p_over().wait_recv()
            total = (ps[at(last), over] + pq[...]).astype(BF16).astype(F32)
            hr[at(last), over] = gelu_tanh(total).astype(BF16)
            h_over().start()
            p_high().wait_recv()
            for k, piece in enumerate(TO_LOW):
                activate(last, pl.ds(*piece))
                h_piece(k, piece).start()

    def own_last():
        multiply(ho, 0, kept, 0, put)

        @pl.when(high)
        def _():
            multiply(ho, kept, SKEW, 0, add)
            multiply(hr, kept, SKEW, half, add)

    def step(t, carry):
        @pl.when(source & (t == 3))
        def _():
            ra[...] = jnp.dot(xv[at(last - 1), :], w1v[0, :, pl.ds(straight, DETOUR)], preferred_element_type=F32)
            detour[0].start()

        @pl.when(relay_high & (t == 4))
        def _():
            detour[0].wait_recv()
            detour[1].start()

        @pl.when(relay_low & (t == 7))
        def _():
            detour[1].wait_recv()
            detour[2].start()

        @pl.when(t < chunks)
        def _():
            partial(t)

        @pl.when(t >= 2)
        def _():
            hidden(t - 2)

        @pl.when(t == chunks)
        def _():
            hidden_last()

        @pl.when(t == 2)
        def _():
            w2_local_all.wait()
            w2_swap_all.wait_recv()

        @pl.when(t >= 2)
        def _():
            second_own(t - 2)

        @pl.when(t == chunks)
        def _():
            own_last()

        @pl.when(t >= 3)
        def _():
            second_layer(t - 3)

        return carry

    lax.fori_loop(1, chunks + 1, step, 0)

    def close(c, term):
        z[pl.ds(2 * M, M), c] = (zs[at(last), c] + term).astype(BF16)

    z_all.wait_recv()

    def came(r, c):
        return zr[pl.ds(r * M, M), c] + zr[pl.ds(rows + r * M, M), c] + zr[pl.ds(2 * rows + r * M, M), c]

    def finish(r, i):
        for n in range(tiles):
            c = pl.ds(n * TILE, TILE)
            z[pl.ds(r * M, M), c] = (zs[at(i), c] + came(r, c)).astype(BF16)

    finish(0, 0)
    for n in range(tiles):
        c = pl.ds(n * TILE, TILE)
        zs[at(last), c] += came(2, c)
    second_other(last - 1)
    finish(1, last - 1)

    def close_pieces(pieces):
        for k, piece in enumerate(pieces):
            h_piece(k, piece).wait_recv()
            multiply(hr, *piece, half, add if k < len(pieces) - 1 else close)

    @pl.when(low)
    def _():
        h_over().wait_recv()
        multiply(ho, kept, SKEW, 0, add)
        close_pieces(TO_LOW)

    @pl.when(high)
    def _():
        close_pieces(TO_HIGH)

    for copy in (x_along_all, x_swap_all, w2_swap_all, x_forward_all, z_all):
        copy.wait_send()
    most = pl.ds(0, (last - 1) * M)
    remote(ps.at[most], pr.at[most], p_send.at[0], p_recv.at[0], across).wait_send()
    most = pl.ds(0, last * M)
    remote(ho.at[most], hr.at[most], h_send.at[0], h_recv.at[0], across).wait_send()

    @pl.when(source)
    def _():
        p_straight().wait_send()
        detour[0].wait_send()

    @pl.when(~source)
    def _():
        p_whole().wait_send()

    @pl.when(low)
    def _():
        p_high().wait_send()
        p_over().wait_send()
        h_piece(0, (0, kept)).wait_send()

    @pl.when(high)
    def _():
        p_low().wait_send()
        h_over().wait_send()
        h_piece(0, (0, half)).wait_send()

    @pl.when(relay_high)
    def _():
        detour[1].wait_send()

    @pl.when(relay_low)
    def _():
        detour[2].wait_send()


def solution(mesh):
    def body(x, w1, w2):
        rows, half = x.shape
        total = 4 * rows
        dma = lambda n: pltpu.SemaphoreType.DMA((n,))
        return pl.pallas_call(
            kernel,
            out_shape=jax.ShapeDtypeStruct((rows, half), BF16),
            in_specs=[pl.BlockSpec(memory_space=pl.ANY)] * 3,
            out_specs=pl.BlockSpec(memory_space=pltpu.VMEM),
            scratch_shapes=[
                pltpu.VMEM((total, half), BF16),
                pltpu.VMEM((2, half, half), BF16),
                pltpu.VMEM((2 * half, half), BF16),
                pltpu.VMEM((total, half), F32),
                pltpu.VMEM((total, half), F32),
                pltpu.VMEM((M, half), F32),
                pltpu.VMEM((total, half), BF16),
                pltpu.VMEM((total, half), BF16),
                pltpu.VMEM((total, half), F32),
                pltpu.VMEM((3 * rows, half), F32),
                pltpu.VMEM((M, DETOUR), F32),
                pltpu.VMEM((M, DETOUR), F32),
                pltpu.VMEM((M, DETOUR), F32),
                pltpu.VMEM((M, SKEW), F32),
                pltpu.VMEM((M, SKEW), F32),
                dma(1), dma(2), dma(1),
                dma(1), dma(1), dma(1), dma(1),
                dma(1), dma(2), dma(1), dma(1),
                dma(4), dma(SLOTS + 1), dma(3), dma(SLOTS + len(TO_LOW) + 1),
                dma(1), dma(1), dma(1), dma(1),
            ],
            compiler_params=pltpu.CompilerParams(
                collective_id=0, has_side_effects=True, vmem_limit_bytes=48 * 1024 * 1024
            ),
        )(pltpu.with_memory_space_constraint(x, pltpu.HBM), w1, w2)

    return jax.shard_map(
        body,
        mesh=mesh,
        in_specs=(P(("cx", "cz"), "cy"), P("cy", ("cz", "cx")), P("cz", ("cy", "cx"))),
        out_specs=P(("cx", "cz"), "cy"),
        check_vma=False,
    )
```

```python
import math

import jax
import jax.numpy as jnp
from jax import lax
from jax.experimental import pallas as pl
from jax.experimental.pallas import tpu as pltpu
from jax.sharding import PartitionSpec as P

MESH = pl.DeviceIdType.MESH
F32 = jnp.float32
BF16 = jnp.bfloat16
M = 64
TILE = 512
FIRST = ((0, 128), (128, 256), (384, 384), (768, 768))
SKEW = 256
TO_LOW = ((0, 768), (768, 512), (1280, 256))
TO_HIGH = ((0, 768), (768, 256), (1024, 256))
SLOTS = 4
DETOUR_LOW, DETOUR_HIGH = 384, 256


def gelu_tanh(c):
    return 0.5 * c * (1.0 + jnp.tanh(math.sqrt(2 / math.pi) * (c + 0.044715 * (c * c * c))))


def kernel(x, w1, w2, z, xv, w1v, w2v, ps, pr, po, ho, hr, zs, zr, ra, rb, rc, pe, pq,
           xl_sem, w1_sem, w2_sem, bx_send, bx_recv, bw_send, bw_recv,
           xy_send, xy_recv, xf_send, xf_recv, p_send, p_recv, h_send, h_recv, z_send, z_recv, r_send, r_recv):
    cz, cy, cx = lax.axis_index("cz"), lax.axis_index("cy"), lax.axis_index("cx")
    across = {"cy": 1 - cy}
    partner = {"cx": 1 - cx}
    along = {"cz": 1 - cz}
    diagonal = {"cz": 1 - cz, "cx": 1 - cx}
    rows, half = x.shape
    chunks = 4 * rows // M
    per = rows // M

    def remote(src, dst, send, recv, device):
        return pltpu.make_async_remote_copy(src_ref=src, dst_ref=dst, send_sem=send, recv_sem=recv,
                                            device_id=device, device_id_type=MESH)

    def at(i, n=M):
        return pl.ds(pl.multiple_of(i * M, M), n)

    last = chunks - 1
    low, high = cy == 0, cy == 1
    kept = half - SKEW
    source, relay = (cz == 0) & (cx == 0), (cz == 1) & (cx == 0)
    sides = ((high, DETOUR_LOW, DETOUR_HIGH), (low, DETOUR_HIGH, DETOUR_LOW))

    x_first = pltpu.make_async_copy(x.at[pl.ds(0, M)], xv.at[pl.ds(0, M)], xl_sem.at[0])
    x_last = pltpu.make_async_copy(x.at[pl.ds(M, rows - M)], xv.at[pl.ds(10 * M, rows - M)], xl_sem.at[0])
    tiles = half // TILE

    def w1_cols(side, start, width):
        return w1.at[:, pl.ds(pl.multiple_of(side * half + start, 128), width)]

    w1_send = [pltpu.make_async_copy(w1_cols(1 - cy, *piece), w1v.at[0, :, pl.ds(*piece)], w1_sem.at[k % 2])
               for k, piece in enumerate(FIRST)]
    w1_keep = pltpu.make_async_copy(w1_cols(cy, 0, half), w1v.at[1], w1_sem.at[0])
    width = w2.shape[1]

    def w2_rows(core, k):
        side = cy if k == 0 else 1 - cy
        return w2.at[pl.ds(pl.multiple_of((core * 2 + side) * half, half), half)]

    mine = pl.ds(pl.multiple_of(cx * width, width), width)
    both = pl.ds(0, 2 * half)
    w2_half = [pl.ds(k * half, half) for k in range(2)]
    w2_local = [pltpu.make_async_copy(w2_rows(cx, k), w2v.at[w2_half[k], mine], w2_sem.at[0]) for k in range(2)]
    w2_local_all = pltpu.make_async_copy(w2.at[both], w2v.at[:, mine], w2_sem.at[0])
    w2_swap = [remote(w2_rows(1 - cx, k), w2v.at[w2_half[k], mine], bw_send.at[0], bw_recv.at[0], partner)
               for k in range(2)]
    w2_swap_all = remote(w2.at[both], w2v.at[:, mine], bw_send.at[0], bw_recv.at[0], partner)
    x_swap = [
        remote(x.at[pl.ds(0, M)], xv.at[pl.ds(M, M)], bx_send.at[0], bx_recv.at[0], partner),
        remote(x.at[pl.ds(M, rows - M)], xv.at[pl.ds(8 * M, rows - M)], bx_send.at[0], bx_recv.at[0], partner),
    ]
    x_swap_all = remote(x, xv.at[pl.ds(7 * M, rows)], bx_send.at[0], bx_recv.at[0], partner)
    x_along = [
        remote(x.at[pl.ds(0, M)], xv.at[pl.ds(2 * M, M)], xy_send.at[0], xy_recv.at[0], along),
        remote(x.at[pl.ds(M, rows - M)], xv.at[pl.ds(3 * M, rows - M)], xy_send.at[0], xy_recv.at[1], along),
    ]
    x_along_all = remote(x, xv.at[pl.ds(2 * M, rows)], xy_send.at[0], xy_recv.at[0], along)
    x_forward = [
        remote(xv.at[pl.ds(2 * M, M)], xv.at[pl.ds(5 * M, M)], xf_send.at[0], xf_recv.at[0], partner),
        remote(xv.at[pl.ds(3 * M, rows - M)], xv.at[pl.ds(6 * M, rows - M)], xf_send.at[0], xf_recv.at[0], partner),
    ]
    x_forward_all = remote(xv.at[pl.ds(2 * M, rows)], xv.at[pl.ds(5 * M, rows)], xf_send.at[0], xf_recv.at[0], partner)

    def p_copy(i):
        return remote(ps.at[at(i)], pr.at[at(i)], p_send.at[0], p_recv.at[i % SLOTS], across)

    def h_copy(i):
        return remote(ho.at[at(i)], hr.at[at(i)], h_send.at[0], h_recv.at[i % SLOTS], across)

    def z_copy(i, slot, row, device):
        return remote(zs.at[at(i)], zr.at[at(slot * per + row)], z_send.at[0], z_recv.at[0], device)

    z_all = remote(zs.at[pl.ds(0, 3 * rows)], zr, z_send.at[0], z_recv.at[0], partner)
    parts = len(FIRST)

    def p_piece(k):
        c = pl.ds(*FIRST[k])
        return remote(ps.at[pl.ds(0, M), c], pr.at[pl.ds(0, M), c], p_send.at[0], p_recv.at[0], across)

    def p_straight(width):
        c = pl.ds(0, half - width)
        return remote(ps.at[at(last - 1), c], pr.at[at(last - 1), c], p_send.at[1], p_recv.at[(last - 1) % SLOTS], across)

    def p_whole():
        return remote(ps.at[at(last - 1)], pr.at[at(last - 1)], p_send.at[1], p_recv.at[(last - 1) % SLOTS], across)

    def p_high():
        return remote(ps.at[at(last)], pr.at[at(last)], p_send.at[2], p_recv.at[last % SLOTS], across)

    def p_over():
        return remote(pe, pq, p_send.at[3], p_recv.at[SLOTS], across)

    def p_low():
        c = pl.ds(0, kept)
        return remote(ps.at[at(last), c], pr.at[at(last), c], p_send.at[2], p_recv.at[last % SLOTS], across)

    def detour(hop, width):
        c, end = pl.ds(0, width), pl.ds(half - width, width)
        if hop == 0:
            return remote(ra.at[:, c], rb.at[:, c], r_send.at[0], r_recv.at[0], along)
        if hop == 1:
            return remote(rb.at[:, c], rc.at[:, c], r_send.at[0], r_recv.at[1], across)
        return remote(rc.at[:, c], pr.at[at(last - 1), end], r_send.at[0], r_recv.at[0], along)

    def h_piece(k, piece):
        c = pl.ds(*piece)
        return remote(ho.at[at(last), c], hr.at[at(last), c], h_send.at[1], h_recv.at[SLOTS + k], across)

    def h_over():
        c = pl.ds(kept, SKEW)
        return remote(hr.at[at(last), c], ho.at[at(last), c], h_send.at[2], h_recv.at[SLOTS + len(TO_LOW)], across)

    barrier = pltpu.get_barrier_semaphore()
    for device in (across, partner, along, diagonal):
        pl.semaphore_signal(barrier, inc=1, device_id=device, device_id_type=MESH)

    x_first.start()
    w1_send[0].start()
    w1_send[1].start()
    x_first.wait()
    for k in range(parts):
        c = pl.ds(*FIRST[k])
        w1_send[k].wait()
        if k < parts - 2:
            w1_send[k + 2].start()
        ps[pl.ds(0, M), c] = jnp.dot(xv[pl.ds(0, M), :], w1v[0, :, c], preferred_element_type=F32)
        if k == 0:
            pl.semaphore_wait(barrier, 4)
        p_piece(k).start()

    x_last.start()
    w1_keep.start()
    for copy in w2_local:
        copy.start()
    x_swap[0].start()
    for copy in x_along:
        copy.start()
    x_swap[1].start()
    for copy in w2_swap:
        copy.start()
    x_last.wait()
    w1_keep.wait()

    def first_layer(i, side, out, out_rows):
        for n in range(half // TILE):
            c = pl.ds(n * TILE, TILE)
            out[out_rows, c] = jnp.dot(xv[at(i), :], w1v[side, :, c], preferred_element_type=F32)

    def partial(i):
        @pl.when(i == 1)
        def _():
            x_swap_all.wait_recv()

        for k in range(2):
            @pl.when(i == 2 + k)
            def _():
                x_along[k].wait_recv()
                x_forward[k].start()

        @pl.when(i == 5)
        def _():
            x_forward_all.wait_recv()

        @pl.when(low & (i == last))
        def _():
            pe[...] = jnp.dot(xv[at(last), :], w1v[1, :, pl.ds(kept, SKEW)], preferred_element_type=F32)
            p_over().start()

        first_layer(i, 0, ps, at(i))

        @pl.when(i < last - 1)
        def _():
            p_copy(i).start()

        for side, width, _ in sides:
            @pl.when(source & side & (i == last - 1))
            def _():
                p_straight(width).start()

        @pl.when(~source & (i == last - 1))
        def _():
            p_whole().start()

        @pl.when(low & (i == last))
        def _():
            p_high().start()

        @pl.when(high & (i == last))
        def _():
            p_low().start()

    def activate(i, c):
        total = (po[:, c] + pr[at(i), c]).astype(BF16).astype(F32)
        ho[at(i), c] = gelu_tanh(total).astype(BF16)

    def hidden(i):
        first_layer(i, 1, po, pl.ds(0, M))

        @pl.when(~source | (i < last - 1))
        def _():
            p_copy(i).wait_recv()

        for side, _, width in sides:
            @pl.when(source & side & (i == last - 1))
            def _():
                p_straight(width).wait_recv()
                detour(2, width).wait_recv()

        for n in range(tiles):
            activate(i, pl.ds(n * TILE, TILE))
        h_copy(i).start()

    def second_own(i):
        for n in range(tiles):
            c = pl.ds(n * TILE, TILE)
            zs[at(i), c] = jnp.dot(ho[at(i), :], w2v[w2_half[0], c], preferred_element_type=F32)

    def second_other(i):
        h_copy(i).wait_recv()
        for n in range(tiles):
            c = pl.ds(n * TILE, TILE)
            zs[at(i), c] += jnp.dot(hr[at(i), :], w2v[w2_half[1], c], preferred_element_type=F32)

    def second_layer(i):
        second_other(i)

        @pl.when(i == 1)
        def _():
            z_copy(i, 0, 0, partner).start()

        @pl.when((i >= 2) & (i < 5))
        def _():
            z_copy(i, 1, i - 2, along).start()

        @pl.when((i >= 5) & (i < 8))
        def _():
            z_copy(i, 2, i - 5, diagonal).start()

        @pl.when((i >= 8) & (i < 10))
        def _():
            z_copy(i, 0, i - 7, partner).start()

    def multiply(h, start, width, below, out):
        for n in range(tiles):
            c = pl.ds(n * TILE, TILE)
            out(c, jnp.dot(h[at(last), pl.ds(start, width)], w2v[pl.ds(below + start, width), c],
                           preferred_element_type=F32))

    def put(c, term):
        zs[at(last), c] = term

    def add(c, term):
        zs[at(last), c] += term

    over = pl.ds(kept, SKEW)

    def hidden_last():
        first_layer(last, 1, po, pl.ds(0, M))

        @pl.when(low)
        def _():
            p_low().wait_recv()
            for k, piece in enumerate(TO_HIGH):
                activate(last, pl.ds(*piece))
                h_piece(k, piece).start()

        @pl.when(high)
        def _():
            p_over().wait_recv()
            total = (ps[at(last), over] + pq[...]).astype(BF16).astype(F32)
            hr[at(last), over] = gelu_tanh(total).astype(BF16)
            h_over().start()
            p_high().wait_recv()
            for k, piece in enumerate(TO_LOW):
                activate(last, pl.ds(*piece))
                h_piece(k, piece).start()

    def own_last():
        multiply(ho, 0, kept, 0, put)

        @pl.when(high)
        def _():
            multiply(ho, kept, SKEW, 0, add)
            multiply(hr, kept, SKEW, half, add)

    def step(t, carry):
        for side, width, back in sides:
            @pl.when(source & side & (t == 3))
            def _():
                end = pl.ds(half - width, width)
                ra[:, pl.ds(0, width)] = jnp.dot(xv[at(last - 1), :], w1v[0, :, end], preferred_element_type=F32)
                detour(0, width).start()

            @pl.when(relay & side & (t == 4))
            def _():
                detour(0, width).wait_recv()
                detour(1, width).start()

            @pl.when(relay & side & (t == 7))
            def _():
                detour(1, back).wait_recv()
                detour(1, width).wait_send()
                detour(2, back).start()

        @pl.when(t < chunks)
        def _():
            partial(t)

        @pl.when(t >= 2)
        def _():
            hidden(t - 2)

        @pl.when(t == chunks)
        def _():
            hidden_last()

        @pl.when(t == 2)
        def _():
            w2_local_all.wait()
            w2_swap_all.wait_recv()

        @pl.when(t >= 2)
        def _():
            second_own(t - 2)

        @pl.when(t == chunks)
        def _():
            own_last()

        @pl.when(t >= 3)
        def _():
            second_layer(t - 3)

        return carry

    lax.fori_loop(1, chunks + 1, step, 0)

    def close(c, term):
        z[pl.ds(2 * M, M), c] = (zs[at(last), c] + term).astype(BF16)

    z_all.wait_recv()

    def came(r, c):
        return zr[pl.ds(r * M, M), c] + zr[pl.ds(rows + r * M, M), c] + zr[pl.ds(2 * rows + r * M, M), c]

    def finish(r, i):
        for n in range(tiles):
            c = pl.ds(n * TILE, TILE)
            z[pl.ds(r * M, M), c] = (zs[at(i), c] + came(r, c)).astype(BF16)

    finish(0, 0)
    for n in range(tiles):
        c = pl.ds(n * TILE, TILE)
        zs[at(last), c] += came(2, c)
    second_other(last - 1)
    finish(1, last - 1)

    def close_pieces(pieces):
        for k, piece in enumerate(pieces):
            h_piece(k, piece).wait_recv()
            multiply(hr, *piece, half, add if k < len(pieces) - 1 else close)

    @pl.when(low)
    def _():
        h_over().wait_recv()
        multiply(ho, kept, SKEW, 0, add)
        close_pieces(TO_LOW)

    @pl.when(high)
    def _():
        close_pieces(TO_HIGH)

    for copy in (x_along_all, x_swap_all, w2_swap_all, x_forward_all, z_all):
        copy.wait_send()
    most = pl.ds(0, (last - 1) * M)
    remote(ps.at[most], pr.at[most], p_send.at[0], p_recv.at[0], across).wait_send()
    most = pl.ds(0, last * M)
    remote(ho.at[most], hr.at[most], h_send.at[0], h_recv.at[0], across).wait_send()

    for side, width, back in sides:
        @pl.when(source & side)
        def _():
            p_straight(width).wait_send()
            detour(0, width).wait_send()

        @pl.when(relay & side)
        def _():
            detour(2, back).wait_send()

    @pl.when(~source)
    def _():
        p_whole().wait_send()

    @pl.when(low)
    def _():
        p_high().wait_send()
        p_over().wait_send()
        h_piece(0, (0, kept)).wait_send()

    @pl.when(high)
    def _():
        p_low().wait_send()
        h_over().wait_send()
        h_piece(0, (0, half)).wait_send()


def solution(mesh):
    def body(x, w1, w2):
        rows, half = x.shape
        total = 4 * rows
        dma = lambda n: pltpu.SemaphoreType.DMA((n,))
        return pl.pallas_call(
            kernel,
            out_shape=jax.ShapeDtypeStruct((rows, half), BF16),
            in_specs=[pl.BlockSpec(memory_space=pl.ANY)] * 3,
            out_specs=pl.BlockSpec(memory_space=pltpu.VMEM),
            scratch_shapes=[
                pltpu.VMEM((total, half), BF16),
                pltpu.VMEM((2, half, half), BF16),
                pltpu.VMEM((2 * half, half), BF16),
                pltpu.VMEM((total, half), F32),
                pltpu.VMEM((total, half), F32),
                pltpu.VMEM((M, half), F32),
                pltpu.VMEM((total, half), BF16),
                pltpu.VMEM((total, half), BF16),
                pltpu.VMEM((total, half), F32),
                pltpu.VMEM((3 * rows, half), F32),
                pltpu.VMEM((M, max(DETOUR_LOW, DETOUR_HIGH)), F32),
                pltpu.VMEM((M, max(DETOUR_LOW, DETOUR_HIGH)), F32),
                pltpu.VMEM((M, max(DETOUR_LOW, DETOUR_HIGH)), F32),
                pltpu.VMEM((M, SKEW), F32),
                pltpu.VMEM((M, SKEW), F32),
                dma(1), dma(2), dma(1),
                dma(1), dma(1), dma(1), dma(1),
                dma(1), dma(2), dma(1), dma(1),
                dma(4), dma(SLOTS + 1), dma(3), dma(SLOTS + len(TO_LOW) + 1),
                dma(1), dma(1), dma(1), dma(2),
            ],
            compiler_params=pltpu.CompilerParams(
                collective_id=0, has_side_effects=True, vmem_limit_bytes=48 * 1024 * 1024
            ),
        )(pltpu.with_memory_space_constraint(x, pltpu.HBM), w1, w2)

    return jax.shard_map(
        body,
        mesh=mesh,
        in_specs=(P(("cx", "cz"), "cy"), P("cy", ("cz", "cx")), P("cz", ("cy", "cx"))),
        out_specs=P(("cx", "cz"), "cy"),
        check_vma=False,
    )
```

```python
import math

import jax
import jax.numpy as jnp
from jax import lax
from jax.experimental import pallas as pl
from jax.experimental.pallas import tpu as pltpu
from jax.sharding import PartitionSpec as P

MESH = pl.DeviceIdType.MESH
F32 = jnp.float32
BF16 = jnp.bfloat16
M = 64
TILE = 512
FIRST = ((0, 128), (128, 256), (384, 384), (768, 768))
SKEW = 256
TO_LOW = ((0, 768), (768, 512), (1280, 256))
TO_HIGH = ((0, 768), (768, 256), (1024, 256))
SLOTS = 4
DETOUR_LOW, DETOUR_HIGH = 384, 256


def gelu_tanh(c):
    return 0.5 * c * (1.0 + jnp.tanh(math.sqrt(2 / math.pi) * (c + 0.044715 * (c * c * c))))


def kernel(x, w1, w2, z, xv, w1v, w2v, ps, pr, po, ho, hr, zs, zr, ra, rb, rc, pe, pq,
           w1_sem, bx_recv, bw_recv,
           xy_send, xy_recv, xf_recv, p_send, p_recv, h_send, h_recv, z_send, z_recv, r_send, r_recv):
    cz, cy, cx = lax.axis_index("cz"), lax.axis_index("cy"), lax.axis_index("cx")
    across = {"cy": 1 - cy}
    partner = {"cx": 1 - cx}
    along = {"cz": 1 - cz}
    diagonal = {"cz": 1 - cz, "cx": 1 - cx}
    rows, half = x.shape
    chunks = 4 * rows // M
    per = rows // M

    def remote(src, dst, send, recv, device):
        return pltpu.make_async_remote_copy(src_ref=src, dst_ref=dst, send_sem=send, recv_sem=recv,
                                            device_id=device, device_id_type=MESH)

    def at(i, n=M):
        return pl.ds(pl.multiple_of(i * M, M), n)

    last = chunks - 1
    low, high = cy == 0, cy == 1
    kept = half - SKEW
    source, relay = (cz == 0) & (cx == 0), (cz == 1) & (cx == 0)
    sides = ((high, DETOUR_LOW, DETOUR_HIGH), (low, DETOUR_HIGH, DETOUR_LOW))

    x_first = pltpu.make_async_copy(x.at[pl.ds(0, M)], xv.at[pl.ds(0, M)], w1_sem.at[2])
    x_last = pltpu.make_async_copy(x.at[pl.ds(M, rows - M)], xv.at[pl.ds(10 * M, rows - M)], w1_sem.at[1])
    tiles = half // TILE

    def w1_cols(side, start, width):
        return w1.at[:, pl.ds(pl.multiple_of(side * half + start, 128), width)]

    w1_send = [pltpu.make_async_copy(w1_cols(1 - cy, *piece), w1v.at[0, :, pl.ds(*piece)], w1_sem.at[k % 2])
               for k, piece in enumerate(FIRST)]
    w1_keep = pltpu.make_async_copy(w1_cols(cy, 0, half), w1v.at[1], w1_sem.at[0])
    width = w2.shape[1]

    def w2_rows(core, k):
        side = cy if k == 0 else 1 - cy
        return w2.at[pl.ds(pl.multiple_of((core * 2 + side) * half, half), half)]

    mine = pl.ds(pl.multiple_of(cx * width, width), width)
    both = pl.ds(0, 2 * half)
    w2_half = [pl.ds(k * half, half) for k in range(2)]
    w2_local = [pltpu.make_async_copy(w2_rows(cx, k), w2v.at[w2_half[k], mine], w1_sem.at[2]) for k in range(2)]
    w2_local_all = pltpu.make_async_copy(w2.at[both], w2v.at[:, mine], w1_sem.at[2])
    w2_swap = [remote(w2_rows(1 - cx, k), w2v.at[w2_half[k], mine], xy_send.at[0], bw_recv.at[0], partner)
               for k in range(2)]
    w2_swap_all = remote(w2.at[both], w2v.at[:, mine], xy_send.at[0], bw_recv.at[0], partner)
    x_swap = [
        remote(x.at[pl.ds(0, M)], xv.at[pl.ds(M, M)], xy_send.at[0], bx_recv.at[0], partner),
        remote(x.at[pl.ds(M, rows - M)], xv.at[pl.ds(8 * M, rows - M)], xy_send.at[0], bx_recv.at[0], partner),
    ]
    x_swap_all = remote(x, xv.at[pl.ds(7 * M, rows)], xy_send.at[0], bx_recv.at[0], partner)
    x_along = [
        remote(x.at[pl.ds(0, M)], xv.at[pl.ds(2 * M, M)], xy_send.at[0], xy_recv.at[0], along),
        remote(x.at[pl.ds(M, rows - M)], xv.at[pl.ds(3 * M, rows - M)], xy_send.at[0], xy_recv.at[1], along),
    ]
    x_forward = [
        remote(xv.at[pl.ds(2 * M, M)], xv.at[pl.ds(5 * M, M)], xy_send.at[0], xf_recv.at[0], partner),
        remote(xv.at[pl.ds(3 * M, rows - M)], xv.at[pl.ds(6 * M, rows - M)], xy_send.at[0], xf_recv.at[0], partner),
    ]
    x_forward_all = remote(xv.at[pl.ds(2 * M, rows)], xv.at[pl.ds(5 * M, rows)], xy_send.at[0], xf_recv.at[0], partner)

    def p_copy(i):
        return remote(ps.at[at(i)], pr.at[at(i)], p_send.at[0], p_recv.at[i % SLOTS], across)

    def h_copy(i):
        return remote(ho.at[at(i)], hr.at[at(i)], h_send.at[0], h_recv.at[i % SLOTS], across)

    def z_copy(i, slot, row, device):
        return remote(zs.at[at(i)], zr.at[at(slot * per + row)], z_send.at[0], z_recv.at[0], device)

    z_all = remote(zs.at[pl.ds(0, 3 * rows)], zr, z_send.at[0], z_recv.at[0], partner)
    parts = len(FIRST)

    def p_piece(k):
        c = pl.ds(*FIRST[k])
        return remote(ps.at[pl.ds(0, M), c], pr.at[pl.ds(0, M), c], p_send.at[0], p_recv.at[0], across)

    def p_straight(width):
        c = pl.ds(0, half - width)
        return remote(ps.at[at(last - 1), c], pr.at[at(last - 1), c], p_send.at[1], p_recv.at[(last - 1) % SLOTS], across)

    def p_whole():
        return remote(ps.at[at(last - 1)], pr.at[at(last - 1)], p_send.at[1], p_recv.at[(last - 1) % SLOTS], across)

    def p_high():
        return remote(ps.at[at(last)], pr.at[at(last)], p_send.at[2], p_recv.at[last % SLOTS], across)

    def p_over():
        return remote(pe, pq, h_send.at[2], h_recv.at[SLOTS + len(TO_LOW)], across)

    def p_low():
        c = pl.ds(0, kept)
        return remote(ps.at[at(last), c], pr.at[at(last), c], p_send.at[2], p_recv.at[last % SLOTS], across)

    def detour(hop, width):
        c, end = pl.ds(0, width), pl.ds(half - width, width)
        if hop == 0:
            return remote(ra.at[:, c], rb.at[:, c], r_send.at[0], r_recv.at[0], along)
        if hop == 1:
            return remote(rb.at[:, c], rc.at[:, c], r_send.at[0], r_recv.at[1], across)
        return remote(rc.at[:, c], pr.at[at(last - 1), end], r_send.at[0], r_recv.at[0], along)

    def h_piece(k, piece):
        c = pl.ds(*piece)
        return remote(ho.at[at(last), c], hr.at[at(last), c], h_send.at[1], h_recv.at[SLOTS + k], across)

    def h_over():
        c = pl.ds(kept, SKEW)
        return remote(hr.at[at(last), c], ho.at[at(last), c], h_send.at[2], h_recv.at[SLOTS + len(TO_LOW)], across)

    barrier = pltpu.get_barrier_semaphore()
    for device in (across, partner, along, diagonal):
        pl.semaphore_signal(barrier, inc=1, device_id=device, device_id_type=MESH)

    x_first.start()
    w1_send[0].start()
    w1_send[1].start()
    x_first.wait()
    for k in range(parts):
        c = pl.ds(*FIRST[k])
        w1_send[k].wait()
        if k < parts - 2:
            w1_send[k + 2].start()
        ps[pl.ds(0, M), c] = jnp.dot(xv[pl.ds(0, M), :], w1v[0, :, c], preferred_element_type=F32)
        if k == 0:
            pl.semaphore_wait(barrier, 4)
        p_piece(k).start()

    x_last.start()
    w1_keep.start()
    for copy in w2_local:
        copy.start()
    x_swap[0].start()
    for copy in x_along:
        copy.start()
    x_swap[1].start()
    for copy in w2_swap:
        copy.start()
    x_last.wait()
    w1_keep.wait()

    def first_layer(i, side, out, out_rows):
        for n in range(half // TILE):
            c = pl.ds(n * TILE, TILE)
            out[out_rows, c] = jnp.dot(xv[at(i), :], w1v[side, :, c], preferred_element_type=F32)

    def partial(i):
        @pl.when(i == 1)
        def _():
            x_swap_all.wait_recv()

        for k in range(2):
            @pl.when(i == 2 + k)
            def _():
                x_along[k].wait_recv()
                x_forward[k].start()

        @pl.when(i == 5)
        def _():
            x_forward_all.wait_recv()

        @pl.when(low & (i == last))
        def _():
            pe[...] = jnp.dot(xv[at(last), :], w1v[1, :, pl.ds(kept, SKEW)], preferred_element_type=F32)
            p_over().start()

        first_layer(i, 0, ps, at(i))

        @pl.when(i < last - 1)
        def _():
            p_copy(i).start()

        for side, width, _ in sides:
            @pl.when(source & side & (i == last - 1))
            def _():
                p_straight(width).start()

        @pl.when(~source & (i == last - 1))
        def _():
            p_whole().start()

        @pl.when(low & (i == last))
        def _():
            p_high().start()

        @pl.when(high & (i == last))
        def _():
            p_low().start()

    def activate(i, c):
        total = (po[:, c] + pr[at(i), c]).astype(BF16).astype(F32)
        ho[at(i), c] = gelu_tanh(total).astype(BF16)

    def hidden(i):
        first_layer(i, 1, po, pl.ds(0, M))

        @pl.when(~source | (i < last - 1))
        def _():
            p_copy(i).wait_recv()

        for side, _, width in sides:
            @pl.when(source & side & (i == last - 1))
            def _():
                p_straight(width).wait_recv()
                detour(2, width).wait_recv()

        for n in range(tiles):
            activate(i, pl.ds(n * TILE, TILE))
        h_copy(i).start()

    def second_own(i):
        for n in range(tiles):
            c = pl.ds(n * TILE, TILE)
            zs[at(i), c] = jnp.dot(ho[at(i), :], w2v[w2_half[0], c], preferred_element_type=F32)

    def second_other(i):
        h_copy(i).wait_recv()
        for n in range(tiles):
            c = pl.ds(n * TILE, TILE)
            zs[at(i), c] += jnp.dot(hr[at(i), :], w2v[w2_half[1], c], preferred_element_type=F32)

    def second_layer(i):
        second_other(i)

        @pl.when(i == 1)
        def _():
            z_copy(i, 0, 0, partner).start()

        @pl.when((i >= 2) & (i < 5))
        def _():
            z_copy(i, 1, i - 2, along).start()

        @pl.when((i >= 5) & (i < 8))
        def _():
            z_copy(i, 2, i - 5, diagonal).start()

        @pl.when((i >= 8) & (i < 10))
        def _():
            z_copy(i, 0, i - 7, partner).start()

    def multiply(h, start, width, below, out):
        for n in range(tiles):
            c = pl.ds(n * TILE, TILE)
            out(c, jnp.dot(h[at(last), pl.ds(start, width)], w2v[pl.ds(below + start, width), c],
                           preferred_element_type=F32))

    def put(c, term):
        zs[at(last), c] = term

    def add(c, term):
        zs[at(last), c] += term

    over = pl.ds(kept, SKEW)

    def hidden_last():
        first_layer(last, 1, po, pl.ds(0, M))

        @pl.when(low)
        def _():
            p_low().wait_recv()
            for k, piece in enumerate(TO_HIGH):
                activate(last, pl.ds(*piece))
                h_piece(k, piece).start()

        @pl.when(high)
        def _():
            p_over().wait_recv()
            total = (ps[at(last), over] + pq[...]).astype(BF16).astype(F32)
            hr[at(last), over] = gelu_tanh(total).astype(BF16)
            h_over().start()
            p_high().wait_recv()
            for k, piece in enumerate(TO_LOW):
                activate(last, pl.ds(*piece))
                h_piece(k, piece).start()

    def own_last():
        multiply(ho, 0, kept, 0, put)

        @pl.when(high)
        def _():
            multiply(ho, kept, SKEW, 0, add)
            multiply(hr, kept, SKEW, half, add)

    def step(t, carry):
        for side, width, back in sides:
            @pl.when(source & side & (t == 3))
            def _():
                end = pl.ds(half - width, width)
                ra[:, pl.ds(0, width)] = jnp.dot(xv[at(last - 1), :], w1v[0, :, end], preferred_element_type=F32)
                detour(0, width).start()

            @pl.when(relay & side & (t == 4))
            def _():
                detour(0, width).wait_recv()
                detour(1, width).start()

            @pl.when(relay & side & (t == 7))
            def _():
                detour(1, back).wait_recv()
                detour(1, width).wait_send()
                detour(2, back).start()

        @pl.when(t < chunks)
        def _():
            partial(t)

        @pl.when(t >= 2)
        def _():
            hidden(t - 2)

        @pl.when(t == chunks)
        def _():
            hidden_last()

        @pl.when(t == 2)
        def _():
            w2_local_all.wait()
            w2_swap_all.wait_recv()

        @pl.when(t >= 2)
        def _():
            second_own(t - 2)

        @pl.when(t == chunks)
        def _():
            own_last()

        @pl.when(t >= 3)
        def _():
            second_layer(t - 3)

        return carry

    lax.fori_loop(1, chunks + 1, step, 0)

    def close(c, term):
        z[pl.ds(2 * M, M), c] = (zs[at(last), c] + term).astype(BF16)

    z_all.wait_recv()

    def came(r, c):
        return zr[pl.ds(r * M, M), c] + zr[pl.ds(rows + r * M, M), c] + zr[pl.ds(2 * rows + r * M, M), c]

    def finish(r, i):
        for n in range(tiles):
            c = pl.ds(n * TILE, TILE)
            z[pl.ds(r * M, M), c] = (zs[at(i), c] + came(r, c)).astype(BF16)

    finish(0, 0)
    for n in range(tiles):
        c = pl.ds(n * TILE, TILE)
        zs[at(last), c] += came(2, c)
    second_other(last - 1)
    finish(1, last - 1)

    def close_pieces(pieces):
        for k, piece in enumerate(pieces):
            h_piece(k, piece).wait_recv()
            multiply(hr, *piece, half, add if k < len(pieces) - 1 else close)

    @pl.when(low)
    def _():
        h_over().wait_recv()
        multiply(ho, kept, SKEW, 0, add)
        close_pieces(TO_LOW)

    @pl.when(high)
    def _():
        close_pieces(TO_HIGH)

    z_all.wait_send()
    sent = pl.ds(0, 3 * rows + half)
    remote(w2v.at[sent], w2v.at[pl.ds(half - 3 * rows, 3 * rows + half)], xy_send.at[0], xy_recv.at[0], along).wait_send()
    most = pl.ds(0, (last - 1) * M)
    remote(ps.at[most], pr.at[most], p_send.at[0], p_recv.at[0], across).wait_send()
    most = pl.ds(0, last * M)
    remote(ho.at[most], hr.at[most], h_send.at[0], h_recv.at[0], across).wait_send()

    for side, width, back in sides:
        @pl.when(source & side)
        def _():
            p_straight(width).wait_send()
            detour(0, width).wait_send()

        @pl.when(relay & side)
        def _():
            detour(2, back).wait_send()

    @pl.when(~source)
    def _():
        p_whole().wait_send()

    @pl.when(low)
    def _():
        p_high().wait_send()
        p_over().wait_send()
        h_piece(0, (0, kept)).wait_send()

    @pl.when(high)
    def _():
        p_low().wait_send()
        h_over().wait_send()
        h_piece(0, (0, half)).wait_send()


def solution(mesh):
    def body(x, w1, w2):
        rows, half = x.shape
        total = 4 * rows
        dma = lambda n: pltpu.SemaphoreType.DMA((n,))
        return pl.pallas_call(
            kernel,
            out_shape=jax.ShapeDtypeStruct((rows, half), BF16),
            in_specs=[pl.BlockSpec(memory_space=pl.ANY)] * 3,
            out_specs=pl.BlockSpec(memory_space=pltpu.VMEM),
            scratch_shapes=[
                pltpu.VMEM((total, half), BF16),
                pltpu.VMEM((2, half, half), BF16),
                pltpu.VMEM((2 * half, half), BF16),
                pltpu.VMEM((total, half), F32),
                pltpu.VMEM((total, half), F32),
                pltpu.VMEM((M, half), F32),
                pltpu.VMEM((total, half), BF16),
                pltpu.VMEM((total, half), BF16),
                pltpu.VMEM((total, half), F32),
                pltpu.VMEM((3 * rows, half), F32),
                pltpu.VMEM((M, max(DETOUR_LOW, DETOUR_HIGH)), F32),
                pltpu.VMEM((M, max(DETOUR_LOW, DETOUR_HIGH)), F32),
                pltpu.VMEM((M, max(DETOUR_LOW, DETOUR_HIGH)), F32),
                pltpu.VMEM((M, SKEW), F32),
                pltpu.VMEM((M, SKEW), F32),
                dma(3),
                dma(1), dma(1),
                dma(1), dma(2), dma(1),
                dma(3), dma(SLOTS), dma(3), dma(SLOTS + len(TO_LOW) + 1),
                dma(1), dma(1), dma(1), dma(2),
            ],
            compiler_params=pltpu.CompilerParams(
                collective_id=0, has_side_effects=True, vmem_limit_bytes=48 * 1024 * 1024
            ),
        )(pltpu.with_memory_space_constraint(x, pltpu.HBM), w1, w2)

    return jax.shard_map(
        body,
        mesh=mesh,
        in_specs=(P(("cx", "cz"), "cy"), P("cy", ("cz", "cx")), P("cz", ("cy", "cx"))),
        out_specs=P(("cx", "cz"), "cy"),
        check_vma=False,
    )
```

```python
import math

import jax
import jax.numpy as jnp
from jax import lax
from jax.experimental import pallas as pl
from jax.experimental.pallas import tpu as pltpu
from jax.sharding import PartitionSpec as P

MESH = pl.DeviceIdType.MESH
F32 = jnp.float32
BF16 = jnp.bfloat16
M = 64
TILE = 512
FIRST = ((0, 128), (128, 256), (384, 384), (768, 768))
SKEW = 256
TO_LOW = ((0, 768), (768, 512), (1280, 256))
TO_HIGH = ((0, 768), (768, 256), (1024, 256))
SLOTS = 4
DETOUR_LOW, DETOUR_HIGH = 384, 128


def gelu_tanh(c):
    return 0.5 * c * (1.0 + jnp.tanh(math.sqrt(2 / math.pi) * (c + 0.044715 * (c * c * c))))


def kernel(x, w1, w2, z, xv, w1v, w2v, ps, pr, po, ho, hr, zs, zr, ra, rb, rc, pe, pq,
           w1_sem, bx_recv, bw_recv,
           xy_send, xy_recv, xf_recv, p_send, p_recv, h_send, h_recv, z_send, z_recv, r_send, r_recv):
    cz, cy, cx = lax.axis_index("cz"), lax.axis_index("cy"), lax.axis_index("cx")
    across = {"cy": 1 - cy}
    partner = {"cx": 1 - cx}
    along = {"cz": 1 - cz}
    diagonal = {"cz": 1 - cz, "cx": 1 - cx}
    rows, half = x.shape
    chunks = 4 * rows // M
    per = rows // M

    def remote(src, dst, send, recv, device):
        return pltpu.make_async_remote_copy(src_ref=src, dst_ref=dst, send_sem=send, recv_sem=recv,
                                            device_id=device, device_id_type=MESH)

    def at(i, n=M):
        return pl.ds(pl.multiple_of(i * M, M), n)

    last = chunks - 1
    low, high = cy == 0, cy == 1
    kept = half - SKEW
    source, relay = (cz == 0) & (cx == 0), (cz == 1) & (cx == 0)
    sides = ((high, DETOUR_LOW, DETOUR_HIGH), (low, DETOUR_HIGH, DETOUR_LOW))

    x_first = pltpu.make_async_copy(x.at[pl.ds(0, M)], xv.at[pl.ds(0, M)], w1_sem.at[2])
    x_last = pltpu.make_async_copy(x.at[pl.ds(M, rows - M)], xv.at[pl.ds(10 * M, rows - M)], w1_sem.at[1])
    tiles = half // TILE

    def w1_cols(side, start, width):
        return w1.at[:, pl.ds(pl.multiple_of(side * half + start, 128), width)]

    w1_send = [pltpu.make_async_copy(w1_cols(1 - cy, *piece), w1v.at[0, :, pl.ds(*piece)], w1_sem.at[k % 2])
               for k, piece in enumerate(FIRST)]
    w1_keep = pltpu.make_async_copy(w1_cols(cy, 0, half), w1v.at[1], w1_sem.at[0])
    width = w2.shape[1]

    def w2_rows(core, k):
        side = cy if k == 0 else 1 - cy
        return w2.at[pl.ds(pl.multiple_of((core * 2 + side) * half, half), half)]

    mine = pl.ds(pl.multiple_of(cx * width, width), width)
    both = pl.ds(0, 2 * half)
    w2_half = [pl.ds(k * half, half) for k in range(2)]
    w2_local = [pltpu.make_async_copy(w2_rows(cx, k), w2v.at[w2_half[k], mine], w1_sem.at[2]) for k in range(2)]
    w2_local_all = pltpu.make_async_copy(w2.at[both], w2v.at[:, mine], w1_sem.at[2])
    w2_swap = [remote(w2_rows(1 - cx, k), w2v.at[w2_half[k], mine], xy_send.at[0], bw_recv.at[0], partner)
               for k in range(2)]
    w2_swap_all = remote(w2.at[both], w2v.at[:, mine], xy_send.at[0], bw_recv.at[0], partner)
    x_swap = [
        remote(x.at[pl.ds(0, M)], xv.at[pl.ds(M, M)], xy_send.at[0], bx_recv.at[0], partner),
        remote(x.at[pl.ds(M, rows - M)], xv.at[pl.ds(8 * M, rows - M)], xy_send.at[0], bx_recv.at[0], partner),
    ]
    x_swap_all = remote(x, xv.at[pl.ds(7 * M, rows)], xy_send.at[0], bx_recv.at[0], partner)
    x_along = [
        remote(x.at[pl.ds(0, M)], xv.at[pl.ds(2 * M, M)], xy_send.at[0], xy_recv.at[0], along),
        remote(x.at[pl.ds(M, rows - M)], xv.at[pl.ds(3 * M, rows - M)], xy_send.at[0], xy_recv.at[1], along),
    ]
    x_forward = [
        remote(xv.at[pl.ds(2 * M, M)], xv.at[pl.ds(5 * M, M)], xy_send.at[0], xf_recv.at[0], partner),
        remote(xv.at[pl.ds(3 * M, rows - M)], xv.at[pl.ds(6 * M, rows - M)], xy_send.at[0], xf_recv.at[0], partner),
    ]
    x_forward_all = remote(xv.at[pl.ds(2 * M, rows)], xv.at[pl.ds(5 * M, rows)], xy_send.at[0], xf_recv.at[0], partner)

    def p_copy(i):
        return remote(ps.at[at(i)], pr.at[at(i)], p_send.at[0], p_recv.at[i % SLOTS], across)

    def h_copy(i):
        return remote(ho.at[at(i)], hr.at[at(i)], h_send.at[0], h_recv.at[i % SLOTS], across)

    def z_copy(i, slot, row, device):
        return remote(zs.at[at(i)], zr.at[at(slot * per + row)], z_send.at[0], z_recv.at[0], device)

    z_all = remote(zs.at[pl.ds(0, 3 * rows)], zr, z_send.at[0], z_recv.at[0], partner)
    parts = len(FIRST)

    def p_piece(k):
        c = pl.ds(*FIRST[k])
        return remote(ps.at[pl.ds(0, M), c], pr.at[pl.ds(0, M), c], p_send.at[0], p_recv.at[0], across)

    def p_straight(width):
        c = pl.ds(0, half - width)
        return remote(ps.at[at(last - 1), c], pr.at[at(last - 1), c], p_send.at[1], p_recv.at[(last - 1) % SLOTS], across)

    def p_whole():
        return remote(ps.at[at(last - 1)], pr.at[at(last - 1)], p_send.at[1], p_recv.at[(last - 1) % SLOTS], across)

    def p_high():
        return remote(ps.at[at(last)], pr.at[at(last)], p_send.at[2], p_recv.at[last % SLOTS], across)

    def p_over():
        return remote(pe, pq, h_send.at[2], h_recv.at[SLOTS + len(TO_LOW)], across)

    def p_low():
        c = pl.ds(0, kept)
        return remote(ps.at[at(last), c], pr.at[at(last), c], p_send.at[2], p_recv.at[last % SLOTS], across)

    def detour(hop, width):
        c, end = pl.ds(0, width), pl.ds(half - width, width)
        if hop == 0:
            return remote(ra.at[:, c], rb.at[:, c], r_send.at[0], r_recv.at[0], along)
        if hop == 1:
            return remote(rb.at[:, c], rc.at[:, c], r_send.at[0], r_recv.at[1], across)
        return remote(rc.at[:, c], pr.at[at(last - 1), end], r_send.at[0], r_recv.at[0], along)

    def h_piece(k, piece):
        c = pl.ds(*piece)
        return remote(ho.at[at(last), c], hr.at[at(last), c], h_send.at[1], h_recv.at[SLOTS + k], across)

    def h_over():
        c = pl.ds(kept, SKEW)
        return remote(hr.at[at(last), c], ho.at[at(last), c], h_send.at[2], h_recv.at[SLOTS + len(TO_LOW)], across)

    barrier = pltpu.get_barrier_semaphore()
    for device in (across, partner, along, diagonal):
        pl.semaphore_signal(barrier, inc=1, device_id=device, device_id_type=MESH)

    x_first.start()
    w1_send[0].start()
    w1_send[1].start()
    x_first.wait()
    for k in range(parts):
        c = pl.ds(*FIRST[k])
        w1_send[k].wait()
        if k < parts - 2:
            w1_send[k + 2].start()
        ps[pl.ds(0, M), c] = jnp.dot(xv[pl.ds(0, M), :], w1v[0, :, c], preferred_element_type=F32)
        if k == 0:
            pl.semaphore_wait(barrier, 4)
        p_piece(k).start()

    x_last.start()
    w1_keep.start()
    for copy in w2_local:
        copy.start()
    x_swap[0].start()
    for copy in x_along:
        copy.start()
    x_swap[1].start()
    for copy in w2_swap:
        copy.start()
    x_last.wait()
    w1_keep.wait()

    def first_layer(i, side, out, out_rows):
        for n in range(half // TILE):
            c = pl.ds(n * TILE, TILE)
            out[out_rows, c] = jnp.dot(xv[at(i), :], w1v[side, :, c], preferred_element_type=F32)

    def partial(i):
        @pl.when(i == 1)
        def _():
            x_swap_all.wait_recv()

        for k in range(2):
            @pl.when(i == 2 + k)
            def _():
                x_along[k].wait_recv()
                x_forward[k].start()

        @pl.when(i == 5)
        def _():
            x_forward_all.wait_recv()

        @pl.when(low & (i == last))
        def _():
            pe[...] = jnp.dot(xv[at(last), :], w1v[1, :, pl.ds(kept, SKEW)], preferred_element_type=F32)
            p_over().start()

        first_layer(i, 0, ps, at(i))

        @pl.when(i < last - 1)
        def _():
            p_copy(i).start()

        for side, width, _ in sides:
            @pl.when(source & side & (i == last - 1))
            def _():
                p_straight(width).start()

        @pl.when(~source & (i == last - 1))
        def _():
            p_whole().start()

        @pl.when(low & (i == last))
        def _():
            p_high().start()

        @pl.when(high & (i == last))
        def _():
            p_low().start()

    def activate(i, c):
        total = (po[:, c] + pr[at(i), c]).astype(BF16).astype(F32)
        ho[at(i), c] = gelu_tanh(total).astype(BF16)

    def hidden(i):
        first_layer(i, 1, po, pl.ds(0, M))

        @pl.when(~source | (i < last - 1))
        def _():
            p_copy(i).wait_recv()

        for side, _, width in sides:
            @pl.when(source & side & (i == last - 1))
            def _():
                p_straight(width).wait_recv()
                detour(2, width).wait_recv()

        for n in range(tiles):
            activate(i, pl.ds(n * TILE, TILE))
        h_copy(i).start()

    def second_own(i):
        for n in range(tiles):
            c = pl.ds(n * TILE, TILE)
            zs[at(i), c] = jnp.dot(ho[at(i), :], w2v[w2_half[0], c], preferred_element_type=F32)

    def second_other(i):
        h_copy(i).wait_recv()
        for n in range(tiles):
            c = pl.ds(n * TILE, TILE)
            zs[at(i), c] += jnp.dot(hr[at(i), :], w2v[w2_half[1], c], preferred_element_type=F32)

    def second_layer(i):
        second_other(i)

        @pl.when(i == 1)
        def _():
            z_copy(i, 0, 0, partner).start()

        @pl.when((i >= 2) & (i < 5))
        def _():
            z_copy(i, 1, i - 2, along).start()

        @pl.when((i >= 5) & (i < 8))
        def _():
            z_copy(i, 2, i - 5, diagonal).start()

        @pl.when((i >= 8) & (i < 10))
        def _():
            z_copy(i, 0, i - 7, partner).start()

    def multiply(h, start, width, below, out):
        for n in range(tiles):
            c = pl.ds(n * TILE, TILE)
            out(c, jnp.dot(h[at(last), pl.ds(start, width)], w2v[pl.ds(below + start, width), c],
                           preferred_element_type=F32))

    def put(c, term):
        zs[at(last), c] = term

    def add(c, term):
        zs[at(last), c] += term

    over = pl.ds(kept, SKEW)

    def hidden_last():
        first_layer(last, 1, po, pl.ds(0, M))

        @pl.when(low)
        def _():
            p_low().wait_recv()
            for k, piece in enumerate(TO_HIGH):
                activate(last, pl.ds(*piece))
                h_piece(k, piece).start()

        @pl.when(high)
        def _():
            p_over().wait_recv()
            total = (ps[at(last), over] + pq[...]).astype(BF16).astype(F32)
            hr[at(last), over] = gelu_tanh(total).astype(BF16)
            h_over().start()
            p_high().wait_recv()
            for k, piece in enumerate(TO_LOW):
                activate(last, pl.ds(*piece))
                h_piece(k, piece).start()

    def own_last():
        multiply(ho, 0, kept, 0, put)

        @pl.when(high)
        def _():
            multiply(ho, kept, SKEW, 0, add)
            multiply(hr, kept, SKEW, half, add)

    def step(t, carry):
        for side, width, back in sides:
            @pl.when(source & side & (t == 3))
            def _():
                end = pl.ds(half - width, width)
                ra[:, pl.ds(0, width)] = jnp.dot(xv[at(last - 1), :], w1v[0, :, end], preferred_element_type=F32)
                detour(0, width).start()

            @pl.when(relay & side & (t == 4))
            def _():
                detour(0, width).wait_recv()
                detour(1, width).start()

            @pl.when(relay & side & (t == 7))
            def _():
                detour(1, back).wait_recv()
                detour(1, width).wait_send()
                detour(2, back).start()

        @pl.when(t < chunks)
        def _():
            partial(t)

        @pl.when(t >= 2)
        def _():
            hidden(t - 2)

        @pl.when(t == chunks)
        def _():
            hidden_last()

        @pl.when(t == 2)
        def _():
            w2_local_all.wait()
            w2_swap_all.wait_recv()

        @pl.when(t >= 2)
        def _():
            second_own(t - 2)

        @pl.when(t == chunks)
        def _():
            own_last()

        @pl.when(t >= 3)
        def _():
            second_layer(t - 3)

        return carry

    lax.fori_loop(1, chunks + 1, step, 0)

    def close(c, term):
        z[pl.ds(2 * M, M), c] = (zs[at(last), c] + term).astype(BF16)

    z_all.wait_recv()

    def came(r, c):
        return zr[pl.ds(r * M, M), c] + zr[pl.ds(rows + r * M, M), c] + zr[pl.ds(2 * rows + r * M, M), c]

    def finish(r, i):
        for n in range(tiles):
            c = pl.ds(n * TILE, TILE)
            z[pl.ds(r * M, M), c] = (zs[at(i), c] + came(r, c)).astype(BF16)

    finish(0, 0)
    for n in range(tiles):
        c = pl.ds(n * TILE, TILE)
        zs[at(last), c] += came(2, c)
    second_other(last - 1)
    finish(1, last - 1)

    def close_pieces(pieces):
        for k, piece in enumerate(pieces):
            h_piece(k, piece).wait_recv()
            multiply(hr, *piece, half, add if k < len(pieces) - 1 else close)

    @pl.when(low)
    def _():
        h_over().wait_recv()
        multiply(ho, kept, SKEW, 0, add)
        close_pieces(TO_LOW)

    @pl.when(high)
    def _():
        close_pieces(TO_HIGH)

    z_all.wait_send()
    sent = pl.ds(0, 3 * rows + half)
    remote(w2v.at[sent], w2v.at[pl.ds(half - 3 * rows, 3 * rows + half)], xy_send.at[0], xy_recv.at[0], along).wait_send()
    most = pl.ds(0, (last - 1) * M)
    remote(ps.at[most], pr.at[most], p_send.at[0], p_recv.at[0], across).wait_send()
    most = pl.ds(0, last * M)
    remote(ho.at[most], hr.at[most], h_send.at[0], h_recv.at[0], across).wait_send()

    for side, width, back in sides:
        @pl.when(source & side)
        def _():
            p_straight(width).wait_send()
            detour(0, width).wait_send()

        @pl.when(relay & side)
        def _():
            detour(2, back).wait_send()

    @pl.when(~source)
    def _():
        p_whole().wait_send()

    @pl.when(low)
    def _():
        p_high().wait_send()
        p_over().wait_send()
        h_piece(0, (0, kept)).wait_send()

    @pl.when(high)
    def _():
        p_low().wait_send()
        h_over().wait_send()
        h_piece(0, (0, half)).wait_send()


def solution(mesh):
    def body(x, w1, w2):
        rows, half = x.shape
        total = 4 * rows
        dma = lambda n: pltpu.SemaphoreType.DMA((n,))
        return pl.pallas_call(
            kernel,
            out_shape=jax.ShapeDtypeStruct((rows, half), BF16),
            in_specs=[pl.BlockSpec(memory_space=pl.ANY)] * 3,
            out_specs=pl.BlockSpec(memory_space=pltpu.VMEM),
            scratch_shapes=[
                pltpu.VMEM((total, half), BF16),
                pltpu.VMEM((2, half, half), BF16),
                pltpu.VMEM((2 * half, half), BF16),
                pltpu.VMEM((total, half), F32),
                pltpu.VMEM((total, half), F32),
                pltpu.VMEM((M, half), F32),
                pltpu.VMEM((total, half), BF16),
                pltpu.VMEM((total, half), BF16),
                pltpu.VMEM((total, half), F32),
                pltpu.VMEM((3 * rows, half), F32),
                pltpu.VMEM((M, max(DETOUR_LOW, DETOUR_HIGH)), F32),
                pltpu.VMEM((M, max(DETOUR_LOW, DETOUR_HIGH)), F32),
                pltpu.VMEM((M, max(DETOUR_LOW, DETOUR_HIGH)), F32),
                pltpu.VMEM((M, SKEW), F32),
                pltpu.VMEM((M, SKEW), F32),
                dma(3),
                dma(1), dma(1),
                dma(1), dma(2), dma(1),
                dma(3), dma(SLOTS), dma(3), dma(SLOTS + len(TO_LOW) + 1),
                dma(1), dma(1), dma(1), dma(2),
            ],
            compiler_params=pltpu.CompilerParams(
                collective_id=0, has_side_effects=True, vmem_limit_bytes=48 * 1024 * 1024
            ),
        )(pltpu.with_memory_space_constraint(x, pltpu.HBM), w1, w2)

    return jax.shard_map(
        body,
        mesh=mesh,
        in_specs=(P(("cx", "cz"), "cy"), P("cy", ("cz", "cx")), P("cz", ("cy", "cx"))),
        out_specs=P(("cx", "cz"), "cy"),
        check_vma=False,
    )
```
